128 devices in a mesh: ops: 16 (over z, x_hi, core), blk: 8 (over y, x_lo).
Axes of the slice: x: 4 (x_hi: 2, x_lo: 2; x = x_hi * 2 + x_lo), y: 4, z: 4, core: 2. Of those that a mesh axis runs over, the one named last changes fastest.
Arguments:
- psi: bfloat16 [2048, 1024], P('blk'), may hold values from -6 to 6
- left_blocks: bfloat16 [256, 16, 128, 128], P('ops', 'blk'), may hold values from -0.5 to 0.5
- right_ops: bfloat16 [256, 1024, 1024], P(('ops', 'blk')), may hold values from -0.046875 to 0.046875
- block_target: int32 [256, 16], P('ops'), may hold values from 0 to 15
- left_partner: int32 [256], P('ops'), may hold values from 0 to 255, as said below
- block_len: int32 [16], replicated, may hold values from 1 to 128, 1536 in all
Outputs:
- sigma: bfloat16 [2048, 1024], P('blk', 'ops')
The draws below stay inside these ranges and needn't reach their ends.
Inputs may be any that keep to these rules, and one draw needn't show every extreme that they name: left_partner is a permutation of 0 to 255 that maps each aligned group of 16 operators onto itself.
All inputs are finite; a program needn't handle non-finite values.
Results may differ from the reference program's by a relative error of at most 0.018.
Values may be sent and summed in bfloat16 or wider, within the bound.
A program may use at most 128 MiB of HBM per device.

```python
import math
import jax
import jax.numpy as jnp
import numpy as np
from jax import lax

BOND = 2048
BS = 128
RW = 1024
NB = 16
K = 256
OPS_GROUP = 16


def draw_left_partner(key, part):
    scores = jax.random.randint(key, (K,), 0, 65536, dtype=jnp.int32) * K + jnp.arange(K, dtype=jnp.int32)
    groups = K // OPS_GROUP
    order = jnp.argsort(scores.reshape(groups, OPS_GROUP), axis=1, stable=True).astype(jnp.int32)
    shifted = order + jnp.arange(groups, dtype=jnp.int32)[:, None] * OPS_GROUP
    return shifted.reshape(K).astype(jnp.int32)


def with_ends(values, stream_key, low, top_value):
    extent = values.shape
    place = [jax.random.randint(jax.random.fold_in(stream_key, axis), (), 0, extent[axis]) for axis in range(len(extent))]
    values = values.at[tuple(place)].set(low)
    longest = extent.index(max(extent))
    place[longest] = (place[longest] + 1) % extent[longest]
    return values.at[tuple(place)].set(top_value)


def with_spikes(array, rng, source, target, parts, factor):
    owner, partner = [(jnp.arange(array.shape[axis_at]) // (array.shape[axis_at] // parts)).reshape([-1 if axis == axis_at else 1 for axis in range(array.ndim)]) for axis_at in (source, target)]
    chosen = jax.random.permutation(rng, parts)[partner]
    strong = (owner == chosen) | (owner == (partner + parts // 2) % parts)
    return jnp.where(strong, factor * array, array)


def level_of(key, extent, split, smallest, top_value):
    factor_of = 1.0
    for position, parts in split:
        draws = jax.random.uniform(jax.random.fold_in(jax.random.fold_in(key, 6), position), (parts,), jnp.float32, smallest / len(split), top_value / len(split))
        factor_of = factor_of * jnp.repeat(jnp.exp(draws), extent[position] // parts).reshape((-1,) + (1,) * (len(extent) - 1 - position))
    return factor_of


def profile(count, total, reach, skew):
    weights = [(1 << 20) // math.isqrt(rank ** skew) + 1 for rank in range(2, count + 1)]
    surplus, holding = total - reach - (count - 1), [1] * (count - 1)
    while surplus > 0:
        candidates = [i for i in range(count - 1) if holding[i] < reach]
        mass, remaining = sum([weights[i] for i in candidates]), surplus
        for i in candidates:
            more = min(reach - holding[i], max(1, remaining * weights[i] // mass), surplus)
            holding[i] = holding[i] + more
            surplus = surplus - more
    return np.array([reach] + holding)


def uneven_parts(stream_key, amount, total, bound, skew):
    if amount == 2:
        one = jax.random.randint(stream_key, (), max(1, total - bound), min(bound, total - 1) + 1)
        return jnp.stack([one, total - one])
    lengths = jnp.asarray(profile(amount, total, bound, skew), jnp.int32)
    couples = (amount - 1) // 2
    source_of, taker = lengths[1:1 + 2 * couples:2], lengths[2:2 + 2 * couples:2]
    room = jnp.minimum(source_of - 1, bound - taker)
    moved = jax.random.randint(jax.random.fold_in(stream_key, 1), (couples,), 0, 1 << 20) % (room + 1)
    lengths = lengths.at[1:1 + 2 * couples:2].set(source_of - moved).at[2:2 + 2 * couples:2].set(taker + moved)
    return lengths[jax.random.permutation(jax.random.fold_in(stream_key, 2), amount)]


def noise(own_key, extent, scale, reach, shards=(), held_as=jnp.bfloat16):
    gain = level_of(own_key, extent, shards, -0.22, 0.18) if shards else 1.0
    values = jax.random.normal(own_key, extent, jnp.float32) * scale * gain
    return jnp.minimum(jnp.maximum(values, -reach), reach).astype(held_as)


def gaussian_with(own_key, shape, spread, limit, shards, heavy, kind=jnp.bfloat16):
    drawn = spread * jax.random.normal(own_key, shape, jnp.float32)
    if shards:
        drawn = drawn * level_of(own_key, shape, shards, -0.22, 0.18)
    return jnp.clip(with_spikes(drawn, jax.random.fold_in(own_key, 3), *heavy), -limit, limit).astype(kind)


def setup_inputs(seed: int = 0) -> dict:
    streams_of = jax.random.split(jax.random.key(seed), 7)
    psi = noise(streams_of[0], (BOND, RW), 1.0, 6.0, ((0, 8),))
    left_blocks = noise(streams_of[1], (K, NB, BS, BS), BS ** -0.5, 0.5, ((0, 16), (1, 8)))
    right_ops = gaussian_with(streams_of[2], (K, RW, RW), (RW * K) ** -0.5, 0.046875, ((0, 128),), (0, 2, 128, 5.5))
    block_target = with_ends(jax.random.randint(streams_of[3], (K, NB), 0, NB), jax.random.fold_in(streams_of[3], 1), 0, NB - 1).astype(jnp.int32)
    left_partner = draw_left_partner(jax.random.fold_in(streams_of[6], 71), 0)
    block_len = uneven_parts(streams_of[5], NB, 3 * BOND // 4, BS, 2).astype(jnp.int32)
    return dict(psi=psi, left_blocks=left_blocks, right_ops=right_ops, block_target=block_target, left_partner=left_partner, block_len=block_len)


def reference(psi, left_blocks, right_ops, block_target, left_partner, block_len):
    nblocks = BOND // BS
    row_index = jnp.arange(BS, dtype=jnp.int32)
    live_rows = row_index[None, :] < block_len[:, None]
    masked = psi.reshape(nblocks, BS, RW) * live_rows[:, :, None].astype(jnp.bfloat16)
    states = masked.reshape(BOND, RW).astype(jnp.float32)

    def absorb(totals, index):
        image = jnp.dot(states, right_ops[index].astype(jnp.float32), precision=lax.Precision.HIGHEST)
        image = lax.optimization_barrier(image.astype(jnp.bfloat16)).astype(jnp.float32)
        image = image.reshape(nblocks, BS, RW)
        owner = left_partner[index]
        mixed = jnp.einsum("qab,qbr->qar", left_blocks[owner].astype(jnp.float32), image, precision=lax.Precision.HIGHEST)
        totals = totals + jax.ops.segment_sum(mixed, block_target[owner], num_segments=nblocks)
        return totals, None

    start = jnp.zeros((nblocks, BS, RW), jnp.float32)
    totals = lax.scan(absorb, start, jnp.arange(K, dtype=jnp.int32))[0]
    result = totals * live_rows[:, :, None].astype(jnp.float32)
    return result.reshape(BOND, RW).astype(jnp.bfloat16)
```

```python
import jax
import jax.numpy as jnp
from jax import lax
from jax.experimental import pallas as pl
from jax.experimental.pallas import tpu as pltpu
from jax.sharding import PartitionSpec as P

MESH = pl.DeviceIdType.MESH
F32, BF16 = jnp.float32, jnp.bfloat16
VMEM, SMEM, DMA = pltpu.VMEM, pltpu.SMEM, pltpu.SemaphoreType.DMA
PZ, PX, PY = 48, 48, 32


def order_kernel(partner, targets, table, fill):
    blk = lax.axis_index("blk")
    owners = [lax.rem(partner[blk * 2 + i], 16) for i in range(2)]
    for t in range(16):
        fill[t] = 0

    @pl.loop(0, 8)
    def _(c):
        for i in range(2):
            for e in range(2):
                t = targets[owners[i], 2 * c + e]
                fill[t] = fill[t] + 1

    begin = jnp.int32(0)
    for t in range(16):
        count = fill[t]
        fill[t] = begin
        table[80 + t] = begin
        table[96 + t] = jnp.where(count > 0, 1, 0)
        begin = begin + count
        table[64 + t] = jnp.maximum(begin - 1, 0)

    @pl.loop(0, 8)
    def _(c):
        for i in range(2):
            for e in range(2):
                t = targets[owners[i], 2 * c + e]
                at = fill[t]
                table[at] = c * 4 + i * 2 + e
                table[32 + at] = jnp.where(at > table[80 + t], 1, 0)
                fill[t] = at + 1


def kernel(
    partner, lens, table, psi, left, right, out,
    states, lsend, lrecv, lin, rops, image, runs, dsend, drecv,
    s1z, s1x, s1y, r1z, r1x, r1y, s2z, s2x, s2y, r2z, r2x, r2y, s3z, s3x, s3y, r3z, r3x, r3y,
    fin, fin_in,
    loc, ysem, xsem, zsem, csem, lsem, dsem, sem1, sem2, sem3, fsem,
):
    ops, blk = lax.axis_index("ops"), lax.axis_index("blk")
    z, xh, core = ops // 4, (ops // 2) % 2, ops % 2
    y, xl = blk // 2, blk % 2
    x, e = xh * 2 + xl, z % 2

    def device(dz=0, dx=0, dy=0, dc=0):
        zz, xx, yy, cc = (z + dz) % 4, (x + dx) % 4, (y + dy) % 4, (core + dc) % 2
        return (zz * 4 + (xx // 2) * 2 + cc, yy * 2 + xx % 2)

    def mate(dy, flip):
        return (ops, ((y + dy) % 4) * 2 + (xl + flip) % 2)

    sent = []

    def send(src, dst, send_sem, recv_sem, to):
        copy = pltpu.make_async_remote_copy(
            src_ref=src, dst_ref=dst, send_sem=send_sem, recv_sem=recv_sem, device_id=to, device_id_type=MESH
        )
        copy.start()
        sent.append(copy)

    def arrived(dst, sem):
        pltpu.make_async_remote_copy(
            src_ref=dst, dst_ref=dst, send_sem=sem, recv_sem=sem, device_id=device(dc=1), device_id_type=MESH
        ).wait_recv()

    in_psi = pltpu.make_async_copy(psi, states.at[pl.ds(blk * 8, 8)], loc.at[0])
    in_left = pltpu.make_async_copy(left, lin, loc.at[1])
    in_right = pltpu.make_async_copy(right, rops, loc.at[2])
    in_psi.start()
    in_left.start()
    in_right.start()

    barrier = pltpu.get_barrier_semaphore()
    peers = [device(dc=1)]
    for d in (1, 2, 3):
        peers += [device(dz=d), device(dx=d), device(dy=d), mate(d, 1)]
    for peer in peers:
        pl.semaphore_signal(barrier, inc=1, device_id=peer, device_id_type=MESH)

    in_left.wait()
    lane = lax.broadcasted_iota(jnp.int32, (128, 128), 1)
    masks = [jnp.where(lane < lens[2 * blk + k], 1.0, 0.0).astype(BF16) for k in range(2)]

    @pl.loop(0, 8)
    def _(c):
        for i in range(2):
            for k in range(2):
                lsend[c, i * 2 + k] = lin[lax.rem(partner[c * 2 + i], 16), k] * masks[k]

    lrecv[blk] = lsend[blk]
    in_psi.wait()
    pl.semaphore_wait(barrier, len(peers))

    ys = [0, 3, 1, 2]

    def unit(j, flip, parity, half, k, n=1):
        c = ((y + ys[j]) % 4) * 2 + (xl + flip) % 2
        return states.at[pl.ds(((c * 2 + parity) * 2 + half) * 2 + k, n)]

    mine = lambda j, flip, k, n=1: unit(j, flip, e, core, k, n)

    send(mine(0, 0, 0, 2), mine(0, 0, 0, 2), ysem.at[0, 0], ysem.at[1, 0], device(dy=1))
    send(mine(0, 0, 0, 2), mine(0, 0, 0, 2), ysem.at[0, 1], ysem.at[1, 1], device(dy=3))

    def x_out(j, k):
        send(mine(j, 0, k), mine(j, 0, k), xsem.at[0, j, k], xsem.at[1, j, k], device(dx=1 if k == 0 else 3))

    def z_out(flip, j, k):
        n = flip * 4 + j
        send(mine(j, flip, k), mine(j, flip, k), zsem.at[0, n, k], zsem.at[1, n, k], device(dz=1 if k == 0 else 3))

    def c_out(flip, j, other):
        n = flip * 4 + j
        ref = unit(j, flip, (e + other) % 2, core, 0, 2)
        send(ref, ref, csem.at[0, n, other], csem.at[1, n, other], device(dc=1))

    def l_out(dy, flip):
        n = dy * 2 + flip
        to = ((y + dy) % 4) * 2 + (xl + flip) % 2
        send(lsend.at[to], lrecv.at[blk], lsem.at[0, n], lsem.at[1, n], mate(dy, flip))

    x_out(0, 0)
    x_out(0, 1)
    l_out(0, 1)
    arrived(mine(1, 0, 0, 2), ysem.at[1, 0])
    send(mine(1, 0, 0), mine(1, 0, 0), ysem.at[0, 2], ysem.at[1, 2], device(dy=1))
    for k in range(2):
        x_out(1, k)
        z_out(0, 1, k)
    c_out(0, 1, 0)
    arrived(mine(2, 0, 0, 2), ysem.at[1, 1])
    send(mine(2, 0, 1), mine(2, 0, 1), ysem.at[0, 3], ysem.at[1, 3], device(dy=3))
    for k in range(2):
        x_out(2, k)
        z_out(0, 2, k)
    c_out(0, 2, 0)
    for dy, flip in ((1, 0), (3, 0), (2, 0), (1, 1), (3, 1), (2, 1)):
        l_out(dy, flip)
    for k in range(2):
        arrived(mine(0, 1, k), xsem.at[1, 0, k])
        z_out(1, 0, k)
    c_out(1, 0, 0)
    for k in range(2):
        arrived(mine(3, 0, k), ysem.at[1, 2 + k])
        x_out(3, k)
        z_out(0, 3, k)
    c_out(0, 3, 0)
    for j in (1, 2, 3):
        for k in range(2):
            arrived(mine(j, 1, k), xsem.at[1, j, k])
            z_out(1, j, k)
        c_out(1, j, 0)
    pieces = [(0, 1), (0, 2), (1, 0), (0, 3), (1, 1), (1, 2), (1, 3)]
    for flip, j in pieces:
        for k in range(2):
            arrived(unit(j, flip, (e + 1) % 2, core, k), zsem.at[1, flip * 4 + j, k])
        c_out(flip, j, 1)
    for flip, j in pieces:
        for other in range(2):
            arrived(unit(j, flip, (e + other) % 2, (core + 1) % 2, 0, 2), csem.at[1, flip * 4 + j, other])
    in_right.wait()

    @pl.loop(0, 8)
    def _(c):
        rows = states[pl.ds(c * 8, 8)].reshape(256, 1024)
        for i in range(2):
            for n in range(4):
                made = jnp.dot(rows, rops[i, :, n * 256 : n * 256 + 256], preferred_element_type=F32).astype(BF16)
                for k in range(2):
                    image[n, c * 4 + i * 2 + k] = made[k * 128 : k * 128 + 128]

    for dy in range(4):
        for flip in range(2):
            if dy or flip:
                source = ((y - dy) % 4) * 2 + (xl + flip) % 2
                arrived(lrecv.at[source], lsem.at[1, dy * 2 + flip])

    def mix(zi):
        chunk = (z + 1 + zi) % 4

        def group(g, acc):
            for u in range(8):
                p = g * 8 + u
                at = table[p]
                keep = table[32 + p].astype(F32)
                acc = acc * keep + jnp.dot(
                    lrecv[at // 4, at % 4], image[chunk, at], preferred_element_type=F32
                )
                runs[zi % 2, p] = acc.astype(BF16)
            return acc

        lax.fori_loop(0, 4, group, jnp.zeros((128, 256), F32))

    def total(zi, t):
        value = runs[zi % 2, table[64 + t]].astype(F32)
        return value * table[96 + t].astype(F32)

    def swap(zi):
        @pl.loop(0, 8)
        def _(c):
            dsend[zi, c] = total(zi, 2 * c + 1 - core).astype(BF16)

    def swap_out(zi):
        send(dsend.at[zi], drecv.at[zi], dsem.at[0, zi], dsem.at[1, zi], device(dc=1))

    def join(zi):
        arrived(drecv.at[zi], dsem.at[1, zi])

        @pl.loop(0, 4)
        def _(yd):
            for xld in range(2):
                c = yd * 2 + xld
                value = (total(zi, 2 * c + core) + drecv[zi, c].astype(F32)).astype(BF16)
                for xhd in range(2):
                    part = value[:, xhd * 128 : xhd * 128 + 128]
                    s1z[zi, (xhd * 2 + xld) * 4 + yd] = part[:PZ]
                    s1x[xhd * 2 + xld, zi, yd] = part[PZ : PZ + PX]
                    s1y[yd, zi, xhd * 2 + xld] = part[PZ + PX :]

    def first_out(zi):
        for d in (1, 2, 3):
            send(s1x.at[(x + d) % 4, zi], r1x.at[d - 1, zi], sem1.at[0, 1, d - 1, zi], sem1.at[1, 1, d - 1, zi], device(dx=d))
            send(s1y.at[(y + d) % 4, zi], r1y.at[d - 1, zi], sem1.at[0, 2, d - 1, zi], sem1.at[1, 2, d - 1, zi], device(dy=d))
        if zi < 3:
            send(s1z.at[zi], r1z.at[zi], sem1.at[0, 0, zi, 0], sem1.at[1, 0, zi, 0], device(dz=zi + 1))

    for zi in range(4):
        mix(zi)
        swap(zi)
        if zi >= 1:
            join(zi - 1)
        swap_out(zi)
        if zi >= 1:
            first_out(zi - 1)
    join(3)
    first_out(3)

    def summed(own, others):
        value = own.astype(F32)
        for other in others:
            value = value + other.astype(F32)
        return value

    for d in range(3):
        arrived(r1z.at[d], sem1.at[1, 0, d, 0])

    @pl.loop(0, 16)
    def _(b):
        s2z[b // 4, b % 4] = summed(s1z[3, b], [r1z[d, b] for d in range(3)]).astype(BF16)

    for d in range(3):
        for zi in range(4):
            arrived(r1x.at[d, zi], sem1.at[1, 1, d, zi])

    @pl.loop(0, 4)
    def _(zi):
        for yd in range(4):
            s2x[yd, zi] = summed(s1x[x, zi, yd], [r1x[d, zi, yd] for d in range(3)]).astype(BF16)

    for d in (1, 2, 3):
        send(s2z.at[(x + d) % 4], r2z.at[d - 1], sem2.at[0, 0, d - 1], sem2.at[1, 0, d - 1], device(dx=d))
    for d in range(3):
        for zi in range(4):
            arrived(r1y.at[d, zi], sem1.at[1, 2, d, zi])

    @pl.loop(0, 4)
    def _(zi):
        for b in range(4):
            s2y[zi, b] = summed(s1y[y, zi, b], [r1y[d, zi, b] for d in range(3)]).astype(BF16)

    for d in (1, 2, 3):
        send(s2x.at[(y + d) % 4], r2x.at[d - 1], sem2.at[0, 1, d - 1], sem2.at[1, 1, d - 1], device(dy=d))

    for d in range(3):
        arrived(r2z.at[d], sem2.at[1, 0, d])
    for yd in range(4):
        s3z[yd] = summed(s2z[x, yd], [r2z[d, yd] for d in range(3)]).astype(BF16)
    for d in range(3):
        send(s2y.at[d], r2y.at[d], sem2.at[0, 2, d], sem2.at[1, 2, d], device(dz=d + 1))
    for d in range(3):
        arrived(r2x.at[d], sem2.at[1, 1, d])
    for zi in range(4):
        s3x[zi] = summed(s2x[y, zi], [r2x[d, zi] for d in range(3)]).astype(BF16)
    for d in (1, 2, 3):
        send(s3z.at[(y + d) % 4], r3z.at[d - 1], sem3.at[0, 0, d - 1], sem3.at[1, 0, d - 1], device(dy=d))
    for d in range(3):
        arrived(r2y.at[d], sem2.at[1, 2, d])
    for b in range(4):
        s3y[b] = summed(s2y[3, b], [r2y[d, b] for d in range(3)]).astype(BF16)
    for d in range(3):
        send(s3x.at[d], r3x.at[d], sem3.at[0, 1, d], sem3.at[1, 1, d], device(dz=d + 1))

    row = lax.broadcasted_iota(jnp.int32, (128, 128), 0)
    live = row < lens[2 * blk + core]
    for d in range(3):
        arrived(r3z.at[d], sem3.at[1, 0, d])
    top = summed(s3z[y], [r3z[d] for d in range(3)])
    for d in (1, 2, 3):
        send(s3y.at[(x + d) % 4], r3y.at[d - 1], sem3.at[0, 2, d - 1], sem3.at[1, 2, d - 1], device(dx=d))
    for d in range(3):
        arrived(r3x.at[d], sem3.at[1, 1, d])
    middle = summed(s3x[3], [r3x[d] for d in range(3)])
    for d in range(3):
        arrived(r3y.at[d], sem3.at[1, 2, d])
    bottom = summed(s3y[x], [r3y[d] for d in range(3)])
    value = jnp.where(live, jnp.concatenate([top, middle, bottom], axis=0), 0.0)
    fin[...] = value.astype(BF16)
    send(fin, fin_in, fsem.at[0], fsem.at[1], device(dc=1))
    pick = lambda a: jnp.where(core == 0, a[:, :64], a[:, 64:])
    out[pl.ds(core * 128, 128), :] = pick(value).astype(BF16)
    arrived(fin_in, fsem.at[1])
    out[pl.ds((1 - core) * 128, 128), :] = pick(fin_in[...].astype(F32)).astype(BF16)
    for copy in sent:
        copy.wait_send()


def local(psi, left_blocks, right_ops, block_target, left_partner, block_len):
    smem = pl.BlockSpec(memory_space=SMEM)
    hbm = pl.BlockSpec(memory_space=pl.ANY)
    table = pl.pallas_call(
        order_kernel,
        name="order",
        out_shape=jax.ShapeDtypeStruct((128,), jnp.int32),
        in_specs=[smem, smem],
        out_specs=smem,
        scratch_shapes=[SMEM((16,), jnp.int32)],
    )(left_partner, block_target)
    b = lambda *shape: VMEM(shape, BF16)
    return pl.pallas_call(
        kernel,
        name="sigma",
        out_shape=jax.ShapeDtypeStruct((256, 64), BF16),
        in_specs=[smem, smem, smem, hbm, hbm, hbm],
        out_specs=pl.BlockSpec(memory_space=VMEM),
        scratch_shapes=[
            b(64, 32, 1024), b(8, 4, 128, 128), b(8, 4, 128, 128), b(16, 2, 128, 128), b(2, 1024, 1024),
            b(4, 32, 128, 256), b(2, 32, 128, 256), b(4, 8, 128, 256), b(4, 8, 128, 256),
            b(4, 16, PZ, 128), b(4, 4, 4, PX, 128), b(4, 4, 4, PY, 128),
            b(3, 16, PZ, 128), b(3, 4, 4, PX, 128), b(3, 4, 4, PY, 128),
            b(4, 4, PZ, 128), b(4, 4, PX, 128), b(4, 4, PY, 128),
            b(3, 4, PZ, 128), b(3, 4, PX, 128), b(3, 4, PY, 128),
            b(4, PZ, 128), b(4, PX, 128), b(4, PY, 128),
            b(3, PZ, 128), b(3, PX, 128), b(3, PY, 128),
            b(128, 128), b(128, 128),
            DMA((3,)), DMA((2, 4)), DMA((2, 4, 2)), DMA((2, 8, 2)), DMA((2, 8, 2)), DMA((2, 8)), DMA((2, 4)),
            DMA((2, 3, 3, 4)), DMA((2, 3, 3)), DMA((2, 3, 3)), DMA((2,)),
        ],
        compiler_params=pltpu.CompilerParams(
            collective_id=0, has_side_effects=True, vmem_limit_bytes=60 << 20
        ),
    )(left_partner, block_len, table, psi.reshape(8, 32, 1024), left_blocks, right_ops)


def solution(mesh):
    return jax.shard_map(
        local,
        mesh=mesh,
        in_specs=(
            P("blk", None),
            P("ops", "blk", None, None),
            P(("ops", "blk"), None, None),
            P("ops", None),
            P("ops"),
            P(),
        ),
        out_specs=P("blk", "ops"),
        check_vma=False,
    )
```

```python
import jax
import jax.numpy as jnp
from jax import lax
from jax.experimental import pallas as pl
from jax.experimental.pallas import tpu as pltpu
from jax.sharding import PartitionSpec as P

MESH = pl.DeviceIdType.MESH
F32, BF16 = jnp.float32, jnp.bfloat16
VMEM, SMEM, DMA = pltpu.VMEM, pltpu.SMEM, pltpu.SemaphoreType.DMA
PZ, PX, PY = 48, 48, 32


def kernel(
    partner, lens, targets, psi, left, right, out,
    states, lsend, lrecv, lin, rops, image, runs, dsend, drecv,
    s1z, s1x, s1y, r1z, r1x, r1y, s2z, s2x, s2y, r2z, r2x, r2y, s3z, s3x, s3y, r3z, r3x, r3y,
    fin, fin_in,
    order, table,
    loc, ysem, xsem, zsem, csem, lsem, dsem, sem1, sem2, sem3, fsem,
):
    ops, blk = lax.axis_index("ops"), lax.axis_index("blk")
    z, xh, core = ops // 4, (ops // 2) % 2, ops % 2
    y, xl = blk // 2, blk % 2
    x, e = xh * 2 + xl, z % 2

    def device(dz=0, dx=0, dy=0, dc=0):
        zz, xx, yy, cc = (z + dz) % 4, (x + dx) % 4, (y + dy) % 4, (core + dc) % 2
        return (zz * 4 + (xx // 2) * 2 + cc, yy * 2 + xx % 2)

    def mate(dy, flip):
        return (ops, ((y + dy) % 4) * 2 + (xl + flip) % 2)

    sent = []

    def send(src, dst, send_sem, recv_sem, to):
        copy = pltpu.make_async_remote_copy(
            src_ref=src, dst_ref=dst, send_sem=send_sem, recv_sem=recv_sem, device_id=to, device_id_type=MESH
        )
        copy.start()
        sent.append(copy)

    def arrived(dst, sem):
        pltpu.make_async_remote_copy(
            src_ref=dst, dst_ref=dst, send_sem=sem, recv_sem=sem, device_id=device(dc=1), device_id_type=MESH
        ).wait_recv()

    barrier = pltpu.get_barrier_semaphore()
    peers = [device(dc=1)]
    for d in (1, 2, 3):
        peers += [device(dz=d), device(dx=d), device(dy=d), mate(d, 1)]
    for peer in peers:
        pl.semaphore_signal(barrier, inc=1, device_id=peer, device_id_type=MESH)
    in_psi = pltpu.make_async_copy(psi, states.at[pl.ds(blk * 8, 8)], loc.at[0])
    in_left = pltpu.make_async_copy(left, lin, loc.at[1])
    in_right = pltpu.make_async_copy(right, rops, loc.at[2])
    in_psi.start()
    in_left.start()
    in_right.start()

    ys = [0, 3, 1, 2]

    def unit(j, flip, parity, half, k, n=1):
        c = ((y + ys[j]) % 4) * 2 + (xl + flip) % 2
        return states.at[pl.ds(((c * 2 + parity) * 2 + half) * 2 + k, n)]

    mine = lambda j, flip, k, n=1: unit(j, flip, e, core, k, n)

    def y_out(n, j, k, dy):
        send(mine(j, 0, k), mine(j, 0, k), ysem.at[0, n], ysem.at[1, n], device(dy=dy))

    def x_out(j, k):
        send(mine(j, 0, k), mine(j, 0, k), xsem.at[0, j, k], xsem.at[1, j, k], device(dx=1 if k == 0 else 3))

    def z_out(flip, j, k):
        n = flip * 4 + j
        send(mine(j, flip, k), mine(j, flip, k), zsem.at[0, n, k], zsem.at[1, n, k], device(dz=1 if k == 0 else 3))

    def c_out(flip, j, other):
        n = flip * 4 + j
        ref = unit(j, flip, (e + other) % 2, core, 0, 2)
        send(ref, ref, csem.at[0, n, other], csem.at[1, n, other], device(dc=1))

    def l_out(dy, flip):
        n = dy * 2 + flip
        to = ((y + dy) % 4) * 2 + (xl + flip) % 2
        send(lsend.at[to], lrecv.at[blk], lsem.at[0, n], lsem.at[1, n], mate(dy, flip))

    def images(*blocks):
        at = [(((y + ys[j]) % 4) * 2 + (xl + flip) % 2) * 2 + (e + other) % 2 for flip, j, other in blocks]

        @pl.loop(0, 2)
        def _(i):
            rows = jnp.concatenate([states[pl.ds(q * 4, 4)].reshape(128, 1024) for q in at], axis=0)
            for n in range(4):
                made = jnp.dot(rows, rops[i, :, n * 256 : n * 256 + 256], preferred_element_type=F32).astype(BF16)
                for k in range(2):
                    image[n, i * 16 + at[k]] = made[k * 128 : k * 128 + 128]

    def images_of(*blocks):
        for flip, j, other in blocks:
            arrived(unit(j, flip, (e + other) % 2, (core + 1) % 2, 0, 2), csem.at[1, flip * 4 + j, other])
        images(*blocks)

    number = lambda cond: jnp.where(cond, 1, 0)
    kk = lax.broadcasted_iota(jnp.int32, (32, 128), 0)
    lane = lax.broadcasted_iota(jnp.int32, (32, 128), 1)
    owners = [lax.rem(partner[blk * 2 + i], 16) for i in range(2)]
    goals = [targets[owners[i], q] for i in range(2) for q in range(16)]
    goal = jnp.zeros((32, 128), jnp.int32)
    for at in range(32):
        goal = jnp.where(kk == at, goals[at], goal)
    key = goal * 32 + kk
    rank, again = jnp.zeros((32, 128), jnp.int32), jnp.zeros((32, 128), jnp.int32)
    for at in range(32):
        rank = rank + number(key > goals[at] * 32 + at)
        again = again + number((goal == goals[at]) & (kk > at))
    place = rank == lane
    left_at = (kk % 16 // 2) * 4 + (kk // 16) * 2 + kk % 2

    def down_sum(value):
        value = value[:8] + value[8:16] + value[16:24] + value[24:]
        return sum(value[r : r + 1] for r in range(1, 8)) + value[:1]

    rows = [
        down_sum(jnp.where(place, kk, 0)), down_sum(jnp.where(place, left_at, 0)),
        down_sum(number(place & (again > 0))), jnp.maximum(down_sum(number(goal <= lane)) - 1, 0),
        jnp.minimum(down_sum(number(goal == lane)), 1), jnp.zeros((3, 128), jnp.int32),
    ]
    order[...] = jnp.concatenate(rows, axis=0)
    order_out = pltpu.make_async_copy(order, table, loc.at[3])

    in_psi.wait()
    pl.semaphore_wait(barrier, len(peers))
    y_out(0, 0, 0, 1)
    y_out(1, 0, 1, 3)
    x_out(0, 0)
    x_out(0, 1)
    y_out(2, 0, 1, 1)
    y_out(3, 0, 0, 3)

    in_left.wait()
    lane = lax.broadcasted_iota(jnp.int32, (128, 128), 1)
    masks = [jnp.where(lane < lens[2 * blk + k], 1.0, 0.0).astype(BF16) for k in range(2)]

    @pl.loop(0, 8)
    def _(c):
        for i in range(2):
            for k in range(2):
                lsend[c, i * 2 + k] = lin[lax.rem(partner[c * 2 + i], 16), k] * masks[k]

    lrecv[blk] = lsend[blk]
    l_out(0, 1)
    order_out.start()
    in_right.wait()

    def from_y(j, k, n):
        arrived(mine(j, 0, k), ysem.at[1, n])
        x_out(j, k)
        z_out(0, j, k)

    def from_x(j, k):
        arrived(mine(j, 1, k), xsem.at[1, j, k])
        z_out(1, j, k)

    def from_z(flip, j):
        for k in range(2):
            arrived(unit(j, flip, (e + 1) % 2, core, k), zsem.at[1, flip * 4 + j, k])
        c_out(flip, j, 1)

    images((0, 0, 0), (0, 0, 1))
    from_y(1, 0, 0)
    y_out(4, 1, 0, 1)
    from_y(2, 1, 1)
    y_out(5, 2, 1, 3)
    from_x(0, 0)
    from_x(0, 1)
    c_out(1, 0, 0)
    from_y(1, 1, 2)
    c_out(0, 1, 0)
    from_y(2, 0, 3)
    c_out(0, 2, 0)
    for dy, flip in ((1, 0), (3, 0), (2, 0), (1, 1), (3, 1), (2, 1)):
        l_out(dy, flip)
    images_of((1, 0, 0), (0, 1, 0))
    from_y(3, 0, 4)
    from_y(3, 1, 5)
    c_out(0, 3, 0)
    from_x(1, 0)
    from_x(2, 1)
    from_x(1, 1)
    c_out(1, 1, 0)
    from_x(2, 0)
    c_out(1, 2, 0)
    from_z(0, 1)
    from_z(0, 2)
    images_of((0, 2, 0), (0, 3, 0))
    from_x(3, 0)
    from_x(3, 1)
    c_out(1, 3, 0)
    from_z(1, 0)
    images_of((0, 1, 1), (0, 2, 1))
    from_z(0, 3)
    images_of((1, 1, 0), (1, 2, 0))
    from_z(1, 1)
    from_z(1, 2)
    images_of((1, 0, 1), (0, 3, 1))
    from_z(1, 3)
    images_of((1, 1, 1), (1, 2, 1))
    images_of((1, 3, 0), (1, 3, 1))
    order_out.wait()
    for dy in range(4):
        for flip in range(2):
            if dy or flip:
                source_at = ((y - dy) % 4) * 2 + (xl + flip) % 2
                arrived(lrecv.at[source_at], lsem.at[1, dy * 2 + flip])

    def mix(zi):
        chunk = (z + 1 + zi) % 4

        def group(g, acc):
            for u in range(8):
                p = g * 8 + u
                keep = table[2, p].astype(F32)
                acc = acc * keep + jnp.dot(
                    lrecv[table[1, p] // 4, table[1, p] % 4], image[chunk, table[0, p]], preferred_element_type=F32
                )
                runs[zi % 2, p] = acc.astype(BF16)
            return acc

        lax.fori_loop(0, 4, group, jnp.zeros((128, 256), F32))

    def total(zi, t):
        value = runs[zi % 2, table[3, t]].astype(F32)
        return value * table[4, t].astype(F32)

    def swap(zi):
        @pl.loop(0, 8)
        def _(c):
            dsend[zi, c] = total(zi, 2 * c + 1 - core).astype(BF16)

    def swap_out(zi):
        send(dsend.at[zi], drecv.at[zi], dsem.at[0, zi], dsem.at[1, zi], device(dc=1))

    def join(zi):
        arrived(drecv.at[zi], dsem.at[1, zi])

        @pl.loop(0, 4)
        def _(yd):
            for xld in range(2):
                c = yd * 2 + xld
                value = (total(zi, 2 * c + core) + drecv[zi, c].astype(F32)).astype(BF16)
                for xhd in range(2):
                    part = value[:, xhd * 128 : xhd * 128 + 128]
                    s1z[zi, (xhd * 2 + xld) * 4 + yd] = part[:PZ]
                    s1x[xhd * 2 + xld, zi, yd] = part[PZ : PZ + PX]
                    s1y[yd, zi, xhd * 2 + xld] = part[PZ + PX :]

    def first_out(zi):
        for d in (1, 2, 3):
            send(s1x.at[(x + d) % 4, zi], r1x.at[d - 1, zi], sem1.at[0, 1, d - 1, zi], sem1.at[1, 1, d - 1, zi], device(dx=d))
            send(s1y.at[(y + d) % 4, zi], r1y.at[d - 1, zi], sem1.at[0, 2, d - 1, zi], sem1.at[1, 2, d - 1, zi], device(dy=d))
        if zi < 3:
            send(s1z.at[zi], r1z.at[zi], sem1.at[0, 0, zi, 0], sem1.at[1, 0, zi, 0], device(dz=zi + 1))

    for zi in range(4):
        mix(zi)
        swap(zi)
        if zi >= 1:
            join(zi - 1)
        swap_out(zi)
        if zi >= 1:
            first_out(zi - 1)
    join(3)
    first_out(3)

    def summed(own, others):
        value = own.astype(F32)
        for other in others:
            value = value + other.astype(F32)
        return value

    for d in range(3):
        arrived(r1z.at[d], sem1.at[1, 0, d, 0])

    @pl.loop(0, 16)
    def _(b):
        s2z[b // 4, b % 4] = summed(s1z[3, b], [r1z[d, b] for d in range(3)]).astype(BF16)

    for d in range(3):
        for zi in range(4):
            arrived(r1x.at[d, zi], sem1.at[1, 1, d, zi])

    @pl.loop(0, 4)
    def _(zi):
        for yd in range(4):
            s2x[yd, zi] = summed(s1x[x, zi, yd], [r1x[d, zi, yd] for d in range(3)]).astype(BF16)

    for d in (1, 2, 3):
        send(s2z.at[(x + d) % 4], r2z.at[d - 1], sem2.at[0, 0, d - 1], sem2.at[1, 0, d - 1], device(dx=d))
    for d in range(3):
        for zi in range(4):
            arrived(r1y.at[d, zi], sem1.at[1, 2, d, zi])

    @pl.loop(0, 4)
    def _(zi):
        for b in range(4):
            s2y[zi, b] = summed(s1y[y, zi, b], [r1y[d, zi, b] for d in range(3)]).astype(BF16)

    for d in (1, 2, 3):
        send(s2x.at[(y + d) % 4], r2x.at[d - 1], sem2.at[0, 1, d - 1], sem2.at[1, 1, d - 1], device(dy=d))

    for d in range(3):
        arrived(r2z.at[d], sem2.at[1, 0, d])
    for yd in range(4):
        s3z[yd] = summed(s2z[x, yd], [r2z[d, yd] for d in range(3)]).astype(BF16)
    for d in range(3):
        send(s2y.at[d], r2y.at[d], sem2.at[0, 2, d], sem2.at[1, 2, d], device(dz=d + 1))
    for d in range(3):
        arrived(r2x.at[d], sem2.at[1, 1, d])
    for zi in range(4):
        s3x[zi] = summed(s2x[y, zi], [r2x[d, zi] for d in range(3)]).astype(BF16)
    for d in (1, 2, 3):
        send(s3z.at[(y + d) % 4], r3z.at[d - 1], sem3.at[0, 0, d - 1], sem3.at[1, 0, d - 1], device(dy=d))
    for d in range(3):
        arrived(r2y.at[d], sem2.at[1, 2, d])
    for b in range(4):
        s3y[b] = summed(s2y[3, b], [r2y[d, b] for d in range(3)]).astype(BF16)
    for d in range(3):
        send(s3x.at[d], r3x.at[d], sem3.at[0, 1, d], sem3.at[1, 1, d], device(dz=d + 1))

    row = lax.broadcasted_iota(jnp.int32, (128, 128), 0)
    live = row < lens[2 * blk + core]
    for d in range(3):
        arrived(r3z.at[d], sem3.at[1, 0, d])
    top = summed(s3z[y], [r3z[d] for d in range(3)])
    for d in (1, 2, 3):
        send(s3y.at[(x + d) % 4], r3y.at[d - 1], sem3.at[0, 2, d - 1], sem3.at[1, 2, d - 1], device(dx=d))
    for d in range(3):
        arrived(r3x.at[d], sem3.at[1, 1, d])
    middle = summed(s3x[3], [r3x[d] for d in range(3)])
    for d in range(3):
        arrived(r3y.at[d], sem3.at[1, 2, d])
    bottom = summed(s3y[x], [r3y[d] for d in range(3)])
    value = jnp.where(live, jnp.concatenate([top, middle, bottom], axis=0), 0.0)
    fin[...] = value.astype(BF16)
    send(fin, fin_in, fsem.at[0], fsem.at[1], device(dc=1))
    pick = lambda a: jnp.where(core == 0, a[:, :64], a[:, 64:])
    out[pl.ds(core * 128, 128), :] = pick(value).astype(BF16)
    arrived(fin_in, fsem.at[1])
    out[pl.ds((1 - core) * 128, 128), :] = pick(fin_in[...].astype(F32)).astype(BF16)
    for copy in sent:
        copy.wait_send()


def local(psi, left_blocks, right_ops, block_target, left_partner, block_len):
    smem = pl.BlockSpec(memory_space=SMEM)
    hbm = pl.BlockSpec(memory_space=pl.ANY)
    b = lambda *shape: VMEM(shape, BF16)
    return pl.pallas_call(
        kernel,
        name="sigma",
        out_shape=jax.ShapeDtypeStruct((256, 64), BF16),
        in_specs=[smem, smem, smem, hbm, hbm, hbm],
        out_specs=pl.BlockSpec(memory_space=VMEM),
        scratch_shapes=[
            b(64, 32, 1024), b(8, 4, 128, 128), b(8, 4, 128, 128), b(16, 2, 128, 128), b(2, 1024, 1024),
            b(4, 32, 128, 256), b(2, 32, 128, 256), b(4, 8, 128, 256), b(4, 8, 128, 256),
            b(4, 16, PZ, 128), b(4, 4, 4, PX, 128), b(4, 4, 4, PY, 128),
            b(3, 16, PZ, 128), b(3, 4, 4, PX, 128), b(3, 4, 4, PY, 128),
            b(4, 4, PZ, 128), b(4, 4, PX, 128), b(4, 4, PY, 128),
            b(3, 4, PZ, 128), b(3, 4, PX, 128), b(3, 4, PY, 128),
            b(4, PZ, 128), b(4, PX, 128), b(4, PY, 128),
            b(3, PZ, 128), b(3, PX, 128), b(3, PY, 128),
            b(128, 128), b(128, 128),
            VMEM((8, 128), jnp.int32), SMEM((8, 128), jnp.int32),
            DMA((4,)), DMA((2, 6)), DMA((2, 4, 2)), DMA((2, 8, 2)), DMA((2, 8, 2)), DMA((2, 8)), DMA((2, 4)),
            DMA((2, 3, 3, 4)), DMA((2, 3, 3)), DMA((2, 3, 3)), DMA((2,)),
        ],
        compiler_params=pltpu.CompilerParams(
            collective_id=0, has_side_effects=True, vmem_limit_bytes=60 << 20
        ),
    )(left_partner, block_len, block_target, psi.reshape(8, 32, 1024), left_blocks, right_ops)


def solution(mesh):
    return jax.shard_map(
        local,
        mesh=mesh,
        in_specs=(
            P("blk", None),
            P("ops", "blk", None, None),
            P(("ops", "blk"), None, None),
            P("ops", None),
            P("ops"),
            P(),
        ),
        out_specs=P("blk", "ops"),
        check_vma=False,
    )
```

```python
import jax
import jax.numpy as jnp
from jax import lax
from jax.experimental import pallas as pl
from jax.experimental.pallas import tpu as pltpu
from jax.sharding import PartitionSpec as P

MESH = pl.DeviceIdType.MESH
F32, BF16 = jnp.float32, jnp.bfloat16
VMEM, SMEM, DMA = pltpu.VMEM, pltpu.SMEM, pltpu.SemaphoreType.DMA
PZ, PX, PY = 32, 48, 48
GROUP = 32
ZR = (1, 3, 2, 0)


def kernel(
    partner, lens, targets, psi, left, right, out,
    states, lsend, lrecv, lin, rops, image, runs, dsend, drecv,
    s1z, s1x, s1y, r1z, r1x, r1y, s2z, s2x, s2y, r2z, r2x, r2y, s3z, s3x, s3y, r3z, r3x, r3y,
    c3z, c3x, c3y,
    order, table,
    loc, ysem, xsem, zsem, csem, lsem, dsem, sem1, sem2, sem2x, sem3s, sem3r, fsem,
):
    ops, blk = lax.axis_index("ops"), lax.axis_index("blk")
    z, xh, core = ops // 4, (ops // 2) % 2, ops % 2
    y, xl = blk // 2, blk % 2
    x, e = xh * 2 + xl, z % 2

    def device(dz=0, dx=0, dy=0, dc=0):
        zz, xx, yy, cc = (z + dz) % 4, (x + dx) % 4, (y + dy) % 4, (core + dc) % 2
        return (zz * 4 + (xx // 2) * 2 + cc, yy * 2 + xx % 2)

    def mate(dy, flip):
        return (ops, ((y + dy) % 4) * 2 + (xl + flip) % 2)

    sent = []

    def send(src, dst, send_sem, recv_sem, to):
        copy = pltpu.make_async_remote_copy(
            src_ref=src, dst_ref=dst, send_sem=send_sem, recv_sem=recv_sem, device_id=to, device_id_type=MESH
        )
        copy.start()
        sent.append(copy)

    def arrived(dst, sem):
        pltpu.make_async_remote_copy(
            src_ref=dst, dst_ref=dst, send_sem=sem, recv_sem=sem, device_id=device(dc=1), device_id_type=MESH
        ).wait_recv()

    barrier = pltpu.get_barrier_semaphore()
    peers = [device(dc=1)]
    for d in (1, 2, 3):
        peers += [device(dc=c, **{axis: d}) for axis in ("dz", "dx", "dy") for c in range(2)] + [mate(d, 1)]
    for peer in peers:
        pl.semaphore_signal(barrier, inc=1, device_id=peer, device_id_type=MESH)
    in_psi = pltpu.make_async_copy(psi, states.at[pl.ds(blk * 8, 8)], loc.at[0])
    in_left = pltpu.make_async_copy(left, lin, loc.at[1])
    in_right = pltpu.make_async_copy(right, rops, loc.at[2])
    in_psi.start()
    in_left.start()
    in_right.start()

    ys = [0, 3, 1, 2]

    def unit(j, flip, parity, half, k, n=1):
        c = ((y + ys[j]) % 4) * 2 + (xl + flip) % 2
        return states.at[pl.ds(((c * 2 + parity) * 2 + half) * 2 + k, n)]

    mine = lambda j, flip, k, n=1: unit(j, flip, e, core, k, n)

    def y_out(n, j, k, dy):
        send(mine(j, 0, k), mine(j, 0, k), ysem.at[0, n], ysem.at[1, n], device(dy=dy))

    def x_out(j, k):
        send(mine(j, 0, k), mine(j, 0, k), xsem.at[0, j, k], xsem.at[1, j, k], device(dx=1 if k == 0 else 3))

    def z_out(flip, j, k):
        n = flip * 4 + j
        send(mine(j, flip, k), mine(j, flip, k), zsem.at[0, n, k], zsem.at[1, n, k], device(dz=1 if k == 0 else 3))

    def c_out(flip, j, other):
        n = flip * 4 + j
        ref = unit(j, flip, (e + other) % 2, core, 0, 2)
        send(ref, ref, csem.at[0, n, other], csem.at[1, n, other], device(dc=1))

    def l_out(dy, flip):
        n = dy * 2 + flip
        to = ((y + dy) % 4) * 2 + (xl + flip) % 2
        send(lsend.at[to], lrecv.at[blk], lsem.at[0, n], lsem.at[1, n], mate(dy, flip))

    def images(*blocks):
        at = [(((y + ys[j]) % 4) * 2 + (xl + flip) % 2) * 2 + (e + other) % 2 for flip, j, other in blocks]

        @pl.loop(0, 2)
        def _(i):
            rows = jnp.concatenate([states[pl.ds(q * 4, 4)].reshape(128, 1024) for q in at], axis=0)
            for n in range(4):
                made = jnp.dot(rows, rops[i, :, n * 256 : n * 256 + 256], preferred_element_type=F32).astype(BF16)
                for k in range(2):
                    image[n, i * 16 + at[k]] = made[k * 128 : k * 128 + 128]

    def images_of(*blocks):
        for flip, j, other in blocks:
            arrived(unit(j, flip, (e + other) % 2, (core + 1) % 2, 0, 2), csem.at[1, flip * 4 + j, other])
        images(*blocks)

    number = lambda cond: jnp.where(cond, 1, 0)
    kk = lax.broadcasted_iota(jnp.int32, (32, 128), 0)
    lane = lax.broadcasted_iota(jnp.int32, (32, 128), 1)
    owners = [lax.rem(partner[blk * 2 + i], 16) for i in range(2)]
    goals = [targets[owners[i], q] for i in range(2) for q in range(16)]
    goal = jnp.zeros((32, 128), jnp.int32)
    for at in range(32):
        goal = jnp.where(kk == at, goals[at], goal)
    key = goal * 32 + kk
    rank, again = jnp.zeros((32, 128), jnp.int32), jnp.zeros((32, 128), jnp.int32)
    for at in range(32):
        rank = rank + number(key > goals[at] * 32 + at)
        again = again + number((goal == goals[at]) & (kk > at))
    place = rank == lane
    left_at = (kk % 16 // 2) * 4 + (kk // 16) * 2 + kk % 2

    def down_sum(value):
        value = value[:8] + value[8:16] + value[16:24] + value[24:]
        return sum(value[r : r + 1] for r in range(1, 8)) + value[:1]

    rows = [
        down_sum(jnp.where(place, kk, 0)), down_sum(jnp.where(place, left_at, 0)),
        down_sum(number(place & (again > 0))), jnp.maximum(down_sum(number(goal <= lane)) - 1, 0),
        jnp.minimum(down_sum(number(goal == lane)), 1), jnp.zeros((3, 128), jnp.int32),
    ]
    order[...] = jnp.concatenate(rows, axis=0)
    order_out = pltpu.make_async_copy(order, table, loc.at[3])

    in_psi.wait()
    pl.semaphore_wait(barrier, len(peers))
    y_out(0, 0, 0, 1)
    y_out(1, 0, 1, 3)
    x_out(0, 0)
    x_out(0, 1)
    y_out(2, 0, 1, 1)
    y_out(3, 0, 0, 3)

    in_left.wait()
    lane = lax.broadcasted_iota(jnp.int32, (128, 128), 1)
    masks = [jnp.where(lane < lens[2 * blk + k], 1.0, 0.0).astype(BF16) for k in range(2)]

    @pl.loop(0, 8)
    def _(c):
        for i in range(2):
            for k in range(2):
                lsend[c, i * 2 + k] = lin[lax.rem(partner[c * 2 + i], 16), k] * masks[k]

    lrecv[blk] = lsend[blk]
    l_out(0, 1)
    order_out.start()
    in_right.wait()

    def from_y(j, k, n):
        arrived(mine(j, 0, k), ysem.at[1, n])
        x_out(j, k)
        z_out(0, j, k)

    def from_x(j, k):
        arrived(mine(j, 1, k), xsem.at[1, j, k])
        z_out(1, j, k)

    def from_z(flip, j):
        for k in range(2):
            arrived(unit(j, flip, (e + 1) % 2, core, k), zsem.at[1, flip * 4 + j, k])
        c_out(flip, j, 1)

    images((0, 0, 0), (0, 0, 1))
    from_y(1, 0, 0)
    y_out(4, 1, 0, 1)
    from_y(2, 1, 1)
    y_out(5, 2, 1, 3)
    from_x(0, 0)
    from_x(0, 1)
    c_out(1, 0, 0)
    from_y(1, 1, 2)
    c_out(0, 1, 0)
    from_y(2, 0, 3)
    c_out(0, 2, 0)
    l_out(1, 0)
    l_out(3, 0)
    l_out(2, 0)
    images_of((1, 0, 0), (0, 1, 0))
    from_y(3, 0, 4)
    from_y(3, 1, 5)
    c_out(0, 3, 0)
    for dy in (1, 3, 2):
        l_out(dy, 1)
    from_x(1, 0)
    from_x(2, 1)
    from_x(1, 1)
    c_out(1, 1, 0)
    from_x(2, 0)
    c_out(1, 2, 0)
    from_z(0, 1)
    from_z(0, 2)
    images_of((0, 2, 0), (0, 3, 0))
    from_x(3, 0)
    from_x(3, 1)
    c_out(1, 3, 0)
    from_z(1, 0)
    images_of((0, 1, 1), (0, 2, 1))
    from_z(0, 3)
    images_of((1, 1, 0), (1, 2, 0))
    from_z(1, 1)
    from_z(1, 2)
    images_of((1, 0, 1), (0, 3, 1))
    from_z(1, 3)
    images_of((1, 1, 1), (1, 2, 1))
    images_of((1, 3, 0), (1, 3, 1))
    order_out.wait()
    for dy in range(4):
        for flip in range(2):
            if dy or flip:
                source_at = ((y - dy) % 4) * 2 + (xl + flip) % 2
                arrived(lrecv.at[source_at], lsem.at[1, dy * 2 + flip])

    def mix(zi):
        chunk = (z + ZR[zi]) % 4

        def group(g, acc):
            for u in range(GROUP):
                p = g * GROUP + u
                keep = table[2, p].astype(F32)
                acc = acc * keep + jnp.dot(
                    lrecv[table[1, p] // 4, table[1, p] % 4], image[chunk, table[0, p]], preferred_element_type=F32
                )
                runs[zi % 2, p] = acc.astype(BF16)
            return acc

        lax.fori_loop(0, 32 // GROUP, group, jnp.zeros((128, 256), F32))

    def total(zi, t):
        value = runs[zi % 2, table[3, t]].astype(F32)
        return value * table[4, t].astype(F32)

    def swap(zi):
        @pl.loop(0, 8)
        def _(c):
            dsend[zi, c] = total(zi, 2 * c + 1 - core).astype(BF16)

    def swap_out(zi):
        send(dsend.at[zi], drecv.at[zi], dsem.at[0, zi], dsem.at[1, zi], device(dc=1))

    def join(zi):
        arrived(drecv.at[zi], dsem.at[1, zi])

        @pl.loop(0, 4)
        def _(yd):
            for xld in range(2):
                c = yd * 2 + xld
                value = (total(zi, 2 * c + core) + drecv[zi, c].astype(F32)).astype(BF16)
                for xhd in range(2):
                    part = value[:, xhd * 128 : xhd * 128 + 128]
                    s1z[zi, (xhd * 2 + xld) * 4 + yd] = part[:PZ]
                    s1x[xhd * 2 + xld, zi, yd] = part[PZ : PZ + PX]
                    s1y[yd, zi, xhd * 2 + xld] = part[PZ + PX :]

    def first_out(zi):
        for d in (1, 2, 3):
            send(s1x.at[(x + d) % 4, zi], r1x.at[d - 1, zi], sem1.at[0, 1, d - 1, zi], sem1.at[1, 1, d - 1, zi], device(dx=d))
            send(s1y.at[(y + d) % 4, zi], r1y.at[d - 1, zi], sem1.at[0, 2, d - 1, zi], sem1.at[1, 2, d - 1, zi], device(dy=d))
        if zi < 3:
            send(s1z.at[zi], r1z.at[zi], sem1.at[0, 0, zi, 0], sem1.at[1, 0, zi, 0], device(dz=ZR[zi]))

    for zi in range(4):
        mix(zi)
        swap(zi)
        swap_out(zi)
        if zi >= 1:
            join(zi - 1)
            first_out(zi - 1)
    join(3)
    first_out(3)

    def summed(own, others):
        value = own.astype(F32)
        for other in others:
            value = value + other.astype(F32)
        return value

    def second_x(zi):
        for d in range(3):
            arrived(r1x.at[d, zi], sem1.at[1, 1, d, zi])
        for yd in range(4):
            s2x[yd, zi] = summed(s1x[x, zi, yd], [r1x[d, zi, yd] for d in range(3)]).astype(BF16)
        for d in (1, 2, 3):
            send(s2x.at[(y + d) % 4, zi], r2x.at[d - 1, zi], sem2x.at[0, d - 1, zi], sem2x.at[1, d - 1, zi], device(dy=d))

    def second_y(zi):
        for d in range(3):
            arrived(r1y.at[d, zi], sem1.at[1, 2, d, zi])
        for b in range(4):
            s2y[zi, b] = summed(s1y[y, zi, b], [r1y[d, zi, b] for d in range(3)]).astype(BF16)
        if zi < 3:
            send(s2y.at[zi], r2y.at[zi], sem2.at[0, 1, zi], sem2.at[1, 1, zi], device(dz=ZR[zi]))

    def second_z():
        for d in range(3):
            arrived(r1z.at[d], sem1.at[1, 0, d, 0])
        for xd in range(4):
            for yd in range(4):
                b = xd * 4 + yd
                s2z[xd, yd] = summed(s1z[3, b], [r1z[d, b] for d in range(3)]).astype(BF16)
        for d in (1, 2, 3):
            send(s2z.at[(x + d) % 4], r2z.at[d - 1], sem2.at[0, 0, d - 1], sem2.at[1, 0, d - 1], device(dx=d))

    def third_out(part, src, dst, d, axis):
        for dc in range(2):
            send(src, dst.at[core, d - 1], sem3s.at[part, dc, d - 1], sem3r.at[part, core, d - 1], device(**{axis: ZR[d - 1] if axis == "dz" else d, "dc": dc}))

    def third_own(part, src, dst):
        send(src, dst, fsem.at[0, part], fsem.at[1, part], device(dc=1))

    def third_x(zi):
        for d in range(3):
            arrived(r2x.at[d, zi], sem2x.at[1, d, zi])
        s3x[zi] = summed(s2x[y, zi], [r2x[d, zi] for d in range(3)]).astype(BF16)
        if zi < 3:
            third_out(1, s3x.at[zi], r3x, zi + 1, "dz")
        else:
            third_own(1, s3x.at[3], c3x)

    second_x(0)
    second_y(0)
    second_x(1)
    second_y(1)
    second_z()
    second_x(2)
    second_y(2)
    third_x(0)
    second_x(3)
    second_y(3)
    third_x(1)
    for d in range(3):
        arrived(r2z.at[d], sem2.at[1, 0, d])
    for yd in range(4):
        s3z[yd] = summed(s2z[x, yd], [r2z[d, yd] for d in range(3)]).astype(BF16)
    for d in (1, 2, 3):
        third_out(0, s3z.at[(y + d) % 4], r3z, d, "dy")
    third_own(0, s3z.at[y], c3z)
    third_x(2)
    for d in range(3):
        arrived(r2y.at[d], sem2.at[1, 1, d])
    for b in range(4):
        s3y[b] = summed(s2y[3, b], [r2y[d, b] for d in range(3)]).astype(BF16)
    for d in (1, 2, 3):
        third_out(2, s3y.at[(x + d) % 4], r3y, d, "dx")
    third_own(2, s3y.at[x], c3y)
    third_x(3)

    row = lax.broadcasted_iota(jnp.int32, (128, 128), 0)
    for part, (got, own) in enumerate(((r3z, c3z), (r3x, c3x), (r3y, c3y))):
        for d in range(3):
            for half in range(2):
                arrived(got.at[half, d], sem3r.at[part, half, d])
        arrived(own, fsem.at[1, part])
    for other in range(2):
        half = (core + other) % 2
        own = (c3z[...], c3x[...], c3y[...]) if other else (s3z[y], s3x[3], s3y[x])
        parts = [summed(a, [got[half, d] for d in range(3)]) for a, got in zip(own, (r3z, r3x, r3y))]
        value = jnp.where(row < lens[2 * blk + half], jnp.concatenate(parts, axis=0), 0.0)
        out[pl.ds(half * 128, 128), :] = jnp.where(core == 0, value[:, :64], value[:, 64:]).astype(BF16)
    for copy in sent:
        copy.wait_send()


def local(psi, left_blocks, right_ops, block_target, left_partner, block_len):
    smem = pl.BlockSpec(memory_space=SMEM)
    hbm = pl.BlockSpec(memory_space=pl.ANY)
    b = lambda *shape: VMEM(shape, BF16)
    return pl.pallas_call(
        kernel,
        name="sigma",
        out_shape=jax.ShapeDtypeStruct((256, 64), BF16),
        in_specs=[smem, smem, smem, hbm, hbm, hbm],
        out_specs=pl.BlockSpec(memory_space=VMEM),
        scratch_shapes=[
            b(64, 32, 1024), b(8, 4, 128, 128), b(8, 4, 128, 128), b(16, 2, 128, 128), b(2, 1024, 1024),
            b(4, 32, 128, 256), b(2, 32, 128, 256), b(4, 8, 128, 256), b(4, 8, 128, 256),
            b(4, 16, PZ, 128), b(4, 4, 4, PX, 128), b(4, 4, 4, PY, 128),
            b(3, 16, PZ, 128), b(3, 4, 4, PX, 128), b(3, 4, 4, PY, 128),
            b(4, 4, PZ, 128), b(4, 4, PX, 128), b(4, 4, PY, 128),
            b(3, 4, PZ, 128), b(3, 4, PX, 128), b(3, 4, PY, 128),
            b(4, PZ, 128), b(4, PX, 128), b(4, PY, 128),
            b(2, 3, PZ, 128), b(2, 3, PX, 128), b(2, 3, PY, 128),
            b(PZ, 128), b(PX, 128), b(PY, 128),
            VMEM((8, 128), jnp.int32), SMEM((8, 128), jnp.int32),
            DMA((4,)), DMA((2, 6)), DMA((2, 4, 2)), DMA((2, 8, 2)), DMA((2, 8, 2)), DMA((2, 8)), DMA((2, 4)),
            DMA((2, 3, 3, 4)), DMA((2, 2, 3)), DMA((2, 3, 4)), DMA((3, 2, 3)), DMA((3, 2, 3)), DMA((2, 3)),
        ],
        compiler_params=pltpu.CompilerParams(
            collective_id=0, has_side_effects=True, vmem_limit_bytes=60 << 20
        ),
    )(left_partner, block_len, block_target, psi.reshape(8, 32, 1024), left_blocks, right_ops)


def solution(mesh):
    return jax.shard_map(
        local,
        mesh=mesh,
        in_specs=(
            P("blk", None),
            P("ops", "blk", None, None),
            P(("ops", "blk"), None, None),
            P("ops", None),
            P("ops"),
            P(),
        ),
        out_specs=P("blk", "ops"),
        check_vma=False,
    )
```

```python
import jax
import jax.numpy as jnp
from jax import lax
from jax.experimental import pallas as pl
from jax.experimental.pallas import tpu as pltpu
from jax.sharding import PartitionSpec as P

MESH = pl.DeviceIdType.MESH
F32, BF16 = jnp.float32, jnp.bfloat16
VMEM, SMEM, DMA = pltpu.VMEM, pltpu.SMEM, pltpu.SemaphoreType.DMA
PZ, PX, PY = 32, 48, 48
GROUP = 32
ZR = (1, 3, 2, 0)


def kernel(
    partner_in, lens_in, targets_in, psi, left, right, out,
    partner, lens, targets,
    states, lsend, lrecv, lin, rops, image, runs, dsend, drecv,
    s1z, s1x, s1y, r1z, r1x, r1y, s2z, s2x, s2y, r2z, r2x, r2y, s3z, s3x, s3y, r3z, r3x, r3y,
    c3z, c3x, c3y,
    order, table,
    loc, ysem, xsem, zsem, csem, lsem, dsem, sem1, sem2, sem2x, sem3s, sem3r, fsem,
):
    ops, blk = lax.axis_index("ops"), lax.axis_index("blk")
    z, xh, core = ops // 4, (ops // 2) % 2, ops % 2
    y, xl = blk // 2, blk % 2
    x, e = xh * 2 + xl, z % 2

    def device(dz=0, dx=0, dy=0, dc=0):
        zz, xx, yy, cc = (z + dz) % 4, (x + dx) % 4, (y + dy) % 4, (core + dc) % 2
        return (zz * 4 + (xx // 2) * 2 + cc, yy * 2 + xx % 2)

    def mate(dy, flip):
        return (ops, ((y + dy) % 4) * 2 + (xl + flip) % 2)

    sent = []

    def send(src, dst, send_sem, recv_sem, to):
        copy = pltpu.make_async_remote_copy(
            src_ref=src, dst_ref=dst, send_sem=send_sem, recv_sem=recv_sem, device_id=to, device_id_type=MESH
        )
        copy.start()
        sent.append(copy)

    def arrived(dst, sem):
        pltpu.make_async_remote_copy(
            src_ref=dst, dst_ref=dst, send_sem=sem, recv_sem=sem, device_id=device(dc=1), device_id_type=MESH
        ).wait_recv()

    barrier = pltpu.get_barrier_semaphore()
    peers = [device(dc=1)]
    for d in (1, 2, 3):
        peers += [device(dc=c, **{axis: d}) for axis in ("dz", "dx", "dy") for c in range(2)] + [mate(d, 1)]
    for peer in peers:
        pl.semaphore_signal(barrier, inc=1, device_id=peer, device_id_type=MESH)
    in_psi = pltpu.make_async_copy(psi, states.at[pl.ds(blk * 16, 16)], loc.at[0])
    in_left = pltpu.make_async_copy(left, lin, loc.at[1])
    in_right = pltpu.make_async_copy(right, rops, loc.at[2])
    small = [
        pltpu.make_async_copy(a, b, loc.at[4 + n])
        for n, (a, b) in enumerate(((partner_in, partner), (lens_in, lens), (targets_in, targets)))
    ]
    in_psi.start()
    for copy in small:
        copy.start()
    in_left.start()
    in_right.start()

    ys = [0, 3, 1, 2]

    def unit(j, flip, parity, half, k, n=1):
        c = ((y + ys[j]) % 4) * 2 + (xl + flip) % 2
        return states.at[pl.ds(((c * 2 + parity) * 2 + half) * 4 + k, n)]

    mine = lambda j, flip, k, n=1: unit(j, flip, e, core, k, n)

    def y_out(n, j, k, dy):
        send(mine(j, 0, k), mine(j, 0, k), ysem.at[0, n], ysem.at[1, n], device(dy=dy))

    def x_out(j, k):
        send(mine(j, 0, k), mine(j, 0, k), xsem.at[0, j, k], xsem.at[1, j, k], device(dx=1 if k < 2 else 3))

    def z_out(flip, j, k):
        n = flip * 4 + j
        send(mine(j, flip, k), mine(j, flip, k), zsem.at[0, n, k], zsem.at[1, n, k], device(dz=1 if k < 2 else 3))

    def c_out(flip, j, other):
        n = flip * 4 + j
        ref = unit(j, flip, (e + other) % 2, core, 0, 4)
        send(ref, ref, csem.at[0, n, other], csem.at[1, n, other], device(dc=1))

    def l_out(dy, flip):
        n = dy * 2 + flip
        to = ((y + dy) % 4) * 2 + (xl + flip) % 2
        send(lsend.at[to], lrecv.at[blk], lsem.at[0, n], lsem.at[1, n], mate(dy, flip))

    def images(*blocks):
        at = [(((y + ys[j]) % 4) * 2 + (xl + flip) % 2) * 2 + (e + other) % 2 for flip, j, other in blocks]

        @pl.loop(0, 2)
        def _(i):
            rows = jnp.concatenate([states[pl.ds(q * 8, 8)].reshape(128, 1024) for q in at], axis=0)
            for n in range(4):
                made = jnp.dot(rows, rops[i, :, n * 256 : n * 256 + 256], preferred_element_type=F32).astype(BF16)
                for k in range(2):
                    image[n, i * 16 + at[k]] = made[k * 128 : k * 128 + 128]

    def images_of(*blocks):
        for flip, j, other in blocks:
            arrived(unit(j, flip, (e + other) % 2, (core + 1) % 2, 0, 4), csem.at[1, flip * 4 + j, other])
        images(*blocks)

    for copy in small:
        copy.wait()
    number = lambda cond: jnp.where(cond, 1, 0)
    kk = lax.broadcasted_iota(jnp.int32, (32, 128), 0)
    lane = lax.broadcasted_iota(jnp.int32, (32, 128), 1)
    owners = [lax.rem(partner[blk * 2 + i], 16) for i in range(2)]
    goals = [targets[owners[i], q] for i in range(2) for q in range(16)]
    goal = jnp.zeros((32, 128), jnp.int32)
    for at in range(32):
        goal = jnp.where(kk == at, goals[at], goal)
    key = goal * 32 + kk
    rank, again = jnp.zeros((32, 128), jnp.int32), jnp.zeros((32, 128), jnp.int32)
    for at in range(32):
        rank = rank + number(key > goals[at] * 32 + at)
        again = again + number((goal == goals[at]) & (kk > at))
    place = rank == lane
    left_at = (kk % 16 // 2) * 4 + (kk // 16) * 2 + kk % 2

    def down_sum(value):
        value = value[:8] + value[8:16] + value[16:24] + value[24:]
        return sum(value[r : r + 1] for r in range(1, 8)) + value[:1]

    rows = [
        down_sum(jnp.where(place, kk, 0)), down_sum(jnp.where(place, left_at, 0)),
        down_sum(number(place & (again > 0))), jnp.maximum(down_sum(number(goal <= lane)) - 1, 0),
        jnp.minimum(down_sum(number(goal == lane)), 1), jnp.zeros((3, 128), jnp.int32),
    ]
    order[...] = jnp.concatenate(rows, axis=0)
    order_out = pltpu.make_async_copy(order, table, loc.at[3])

    in_psi.wait()
    pl.semaphore_wait(barrier, len(peers))
    for k in range(4):
        y_out(k, 0, k, 1)
        y_out(7 - k, 0, 3 - k, 3)
        x_out(0, (0, 2, 1, 3)[k])

    in_left.wait()
    lane = lax.broadcasted_iota(jnp.int32, (128, 128), 1)
    masks = [jnp.where(lane < lens[2 * blk + k], 1.0, 0.0).astype(BF16) for k in range(2)]

    @pl.loop(0, 8)
    def _(c):
        for i in range(2):
            for k in range(2):
                lsend[c, i * 2 + k] = lin[lax.rem(partner[c * 2 + i], 16), k] * masks[k]

    lrecv[blk] = lsend[blk]
    l_out(0, 1)
    order_out.start()
    in_right.wait()

    def from_y(j, k, n):
        arrived(mine(j, 0, k), ysem.at[1, n])
        x_out(j, k)
        z_out(0, j, k)

    def near_y(k):
        arrived(mine(1, 0, k), ysem.at[1, k])
        if k < 2:
            y_out(8 + k, 1, k, 1)
        x_out(1, k)
        z_out(0, 1, k)
        m = 3 - k
        arrived(mine(2, 0, m), ysem.at[1, 4 + m])
        if m > 1:
            y_out(8 + m, 2, m, 3)
        x_out(2, m)
        z_out(0, 2, m)

    def from_x(j, k):
        arrived(mine(j, 1, k), xsem.at[1, j, k])
        z_out(1, j, k)

    def from_z(flip, j):
        for k in range(4):
            arrived(unit(j, flip, (e + 1) % 2, core, k), zsem.at[1, flip * 4 + j, k])
        c_out(flip, j, 1)

    images((0, 0, 0), (0, 0, 1))
    near_y(0)
    near_y(1)
    for k in range(4):
        from_x(0, k)
    c_out(1, 0, 0)
    near_y(2)
    near_y(3)
    c_out(0, 1, 0)
    c_out(0, 2, 0)
    l_out(1, 0)
    l_out(3, 0)
    l_out(2, 0)
    for k in (0, 3, 1, 2):
        from_y(3, k, 8 + k)
    c_out(0, 3, 0)
    for dy in (1, 3, 2):
        l_out(dy, 1)
    images_of((1, 0, 0), (0, 1, 0))
    for k in range(4):
        from_x(1, k)
        from_x(2, 3 - k)
    c_out(1, 1, 0)
    c_out(1, 2, 0)
    from_z(0, 1)
    from_z(0, 2)
    images_of((0, 2, 0), (0, 3, 0))
    for k in (0, 3, 1, 2):
        from_x(3, k)
    c_out(1, 3, 0)
    from_z(1, 0)
    images_of((0, 1, 1), (0, 2, 1))
    from_z(0, 3)
    images_of((1, 1, 0), (1, 2, 0))
    from_z(1, 1)
    from_z(1, 2)
    images_of((1, 0, 1), (0, 3, 1))
    from_z(1, 3)
    images_of((1, 1, 1), (1, 2, 1))
    images_of((1, 3, 0), (1, 3, 1))
    order_out.wait()
    for dy in range(4):
        for flip in range(2):
            if dy or flip:
                source_at = ((y - dy) % 4) * 2 + (xl + flip) % 2
                arrived(lrecv.at[source_at], lsem.at[1, dy * 2 + flip])

    def mix(zi):
        chunk = (z + ZR[zi]) % 4

        def group(g, acc):
            for u in range(GROUP):
                p = g * GROUP + u
                keep = table[2, p].astype(F32)
                acc = acc * keep + jnp.dot(
                    lrecv[table[1, p] // 4, table[1, p] % 4], image[chunk, table[0, p]], preferred_element_type=F32
                )
                runs[zi % 2, p] = acc.astype(BF16)
            return acc

        lax.fori_loop(0, 32 // GROUP, group, jnp.zeros((128, 256), F32))

    def total(zi, t):
        value = runs[zi % 2, table[3, t]].astype(F32)
        return value * table[4, t].astype(F32)

    def swap(zi):
        @pl.loop(0, 8)
        def _(c):
            dsend[zi, c] = total(zi, 2 * c + 1 - core).astype(BF16)

    def swap_out(zi):
        send(dsend.at[zi], drecv.at[zi], dsem.at[0, zi], dsem.at[1, zi], device(dc=1))

    def join(zi):
        arrived(drecv.at[zi], dsem.at[1, zi])

        @pl.loop(0, 4)
        def _(yd):
            for xld in range(2):
                c = yd * 2 + xld
                value = (total(zi, 2 * c + core) + drecv[zi, c].astype(F32)).astype(BF16)
                for xhd in range(2):
                    part = value[:, xhd * 128 : xhd * 128 + 128]
                    s1z[zi, (xhd * 2 + xld) * 4 + yd] = part[:PZ]
                    s1x[xhd * 2 + xld, zi, yd] = part[PZ : PZ + PX]
                    s1y[yd, zi, xhd * 2 + xld] = part[PZ + PX :]

    def first_out(zi):
        for d in (1, 2, 3):
            send(s1x.at[(x + d) % 4, zi], r1x.at[d - 1, zi], sem1.at[0, 1, d - 1, zi], sem1.at[1, 1, d - 1, zi], device(dx=d))
            send(s1y.at[(y + d) % 4, zi], r1y.at[d - 1, zi], sem1.at[0, 2, d - 1, zi], sem1.at[1, 2, d - 1, zi], device(dy=d))
        if zi < 3:
            send(s1z.at[zi], r1z.at[zi], sem1.at[0, 0, zi, 0], sem1.at[1, 0, zi, 0], device(dz=ZR[zi]))

    for zi in range(4):
        mix(zi)
        swap(zi)
        swap_out(zi)
        if zi >= 1:
            join(zi - 1)
            first_out(zi - 1)
    join(3)
    first_out(3)

    def summed(own, others):
        value = own.astype(F32)
        for other in others:
            value = value + other.astype(F32)
        return value

    def second_x(zi):
        for d in range(3):
            arrived(r1x.at[d, zi], sem1.at[1, 1, d, zi])
        for yd in range(4):
            s2x[yd, zi] = summed(s1x[x, zi, yd], [r1x[d, zi, yd] for d in range(3)]).astype(BF16)
        for d in (1, 2, 3):
            send(s2x.at[(y + d) % 4, zi], r2x.at[d - 1, zi], sem2x.at[0, d - 1, zi], sem2x.at[1, d - 1, zi], device(dy=d))

    def second_y(zi):
        for d in range(3):
            arrived(r1y.at[d, zi], sem1.at[1, 2, d, zi])
        for b in range(4):
            s2y[zi, b] = summed(s1y[y, zi, b], [r1y[d, zi, b] for d in range(3)]).astype(BF16)
        if zi < 3:
            send(s2y.at[zi], r2y.at[zi], sem2.at[0, 1, zi], sem2.at[1, 1, zi], device(dz=ZR[zi]))

    def second_z():
        for d in range(3):
            arrived(r1z.at[d], sem1.at[1, 0, d, 0])
        for xd in range(4):
            for yd in range(4):
                b = xd * 4 + yd
                s2z[xd, yd] = summed(s1z[3, b], [r1z[d, b] for d in range(3)]).astype(BF16)
        for d in (1, 2, 3):
            send(s2z.at[(x + d) % 4], r2z.at[d - 1], sem2.at[0, 0, d - 1], sem2.at[1, 0, d - 1], device(dx=d))

    def third_out(part, src, dst, d, axis):
        for dc in range(2):
            send(src, dst.at[core, d - 1], sem3s.at[part, dc, d - 1], sem3r.at[part, core, d - 1], device(**{axis: ZR[d - 1] if axis == "dz" else d, "dc": dc}))

    def third_own(part, src, dst):
        send(src, dst, fsem.at[0, part], fsem.at[1, part], device(dc=1))

    def third_x(zi):
        for d in range(3):
            arrived(r2x.at[d, zi], sem2x.at[1, d, zi])
        s3x[zi] = summed(s2x[y, zi], [r2x[d, zi] for d in range(3)]).astype(BF16)
        if zi < 3:
            third_out(1, s3x.at[zi], r3x, zi + 1, "dz")
        else:
            third_own(1, s3x.at[3], c3x)

    second_x(0)
    second_y(0)
    second_x(1)
    second_y(1)
    second_z()
    second_x(2)
    second_y(2)
    third_x(0)
    second_x(3)
    second_y(3)
    third_x(1)
    for d in range(3):
        arrived(r2z.at[d], sem2.at[1, 0, d])
    for yd in range(4):
        s3z[yd] = summed(s2z[x, yd], [r2z[d, yd] for d in range(3)]).astype(BF16)
    for d in (1, 2, 3):
        third_out(0, s3z.at[(y + d) % 4], r3z, d, "dy")
    third_own(0, s3z.at[y], c3z)
    third_x(2)
    for d in range(3):
        arrived(r2y.at[d], sem2.at[1, 1, d])
    for b in range(4):
        s3y[b] = summed(s2y[3, b], [r2y[d, b] for d in range(3)]).astype(BF16)
    for d in (1, 2, 3):
        third_out(2, s3y.at[(x + d) % 4], r3y, d, "dx")
    third_own(2, s3y.at[x], c3y)
    third_x(3)

    row = lax.broadcasted_iota(jnp.int32, (128, 128), 0)
    for part, (got, own) in enumerate(((r3z, c3z), (r3x, c3x), (r3y, c3y))):
        for d in range(3):
            for half in range(2):
                arrived(got.at[half, d], sem3r.at[part, half, d])
        arrived(own, fsem.at[1, part])
    for other in range(2):
        half = (core + other) % 2
        own = (c3z[...], c3x[...], c3y[...]) if other else (s3z[y], s3x[3], s3y[x])
        parts = [summed(a, [got[half, d] for d in range(3)]) for a, got in zip(own, (r3z, r3x, r3y))]
        value = jnp.where(row < lens[2 * blk + half], jnp.concatenate(parts, axis=0), 0.0)
        turned = value.T
        out[:, pl.ds(pl.multiple_of(half * 128, 128), 128)] = jnp.where(core == 0, turned[:64], turned[64:]).astype(BF16)
    for copy in sent:
        copy.wait_send()


def local(psi, left_blocks, right_ops, block_target, left_partner, block_len):
    hbm = pl.BlockSpec(memory_space=pl.ANY)
    b = lambda *shape: VMEM(shape, BF16)
    return pl.pallas_call(
        kernel,
        name="sigma",
        out_shape=jax.ShapeDtypeStruct((64, 256), BF16),
        in_specs=[hbm] * 6,
        out_specs=pl.BlockSpec(memory_space=VMEM),
        scratch_shapes=[
            SMEM((16,), jnp.int32), SMEM((16,), jnp.int32), SMEM((16, 16), jnp.int32),
            b(128, 16, 1024), b(8, 4, 128, 128), b(8, 4, 128, 128), b(16, 2, 128, 128), b(2, 1024, 1024),
            b(4, 32, 128, 256), b(2, 32, 128, 256), b(4, 8, 128, 256), b(4, 8, 128, 256),
            b(4, 16, PZ, 128), b(4, 4, 4, PX, 128), b(4, 4, 4, PY, 128),
            b(3, 16, PZ, 128), b(3, 4, 4, PX, 128), b(3, 4, 4, PY, 128),
            b(4, 4, PZ, 128), b(4, 4, PX, 128), b(4, 4, PY, 128),
            b(3, 4, PZ, 128), b(3, 4, PX, 128), b(3, 4, PY, 128),
            b(4, PZ, 128), b(4, PX, 128), b(4, PY, 128),
            b(2, 3, PZ, 128), b(2, 3, PX, 128), b(2, 3, PY, 128),
            b(PZ, 128), b(PX, 128), b(PY, 128),
            VMEM((8, 128), jnp.int32), SMEM((8, 128), jnp.int32),
            DMA((7,)), DMA((2, 12)), DMA((2, 4, 4)), DMA((2, 8, 4)), DMA((2, 8, 2)), DMA((2, 8)), DMA((2, 4)),
            DMA((2, 3, 3, 4)), DMA((2, 2, 3)), DMA((2, 3, 4)), DMA((3, 2, 3)), DMA((3, 2, 3)), DMA((2, 3)),
        ],
        compiler_params=pltpu.CompilerParams(
            collective_id=0, has_side_effects=True, vmem_limit_bytes=60 << 20
        ),
    )(left_partner, block_len, block_target, psi.reshape(16, 16, 1024), left_blocks, right_ops).T


def solution(mesh):
    return jax.shard_map(
        local,
        mesh=mesh,
        in_specs=(
            P("blk", None),
            P("ops", "blk", None, None),
            P(("ops", "blk"), None, None),
            P("ops", None),
            P("ops"),
            P(),
        ),
        out_specs=P("blk", "ops"),
        check_vma=False,
    )
```

```python
import jax
import jax.numpy as jnp
from jax import lax
from jax.experimental import pallas as pl
from jax.experimental.pallas import tpu as pltpu
from jax.sharding import PartitionSpec as P

MESH = pl.DeviceIdType.MESH
F32, BF16 = jnp.float32, jnp.bfloat16
VMEM, SMEM, DMA = pltpu.VMEM, pltpu.SMEM, pltpu.SemaphoreType.DMA
PZ, PX, PY = 32, 48, 48
GROUP = 32
ZR = (1, 3, 2, 0)


def kernel(
    partner_in, lens_in, targets_in, psi, left, right, out,
    partner, lens, targets,
    states, lsend, lrecv, lin, rops, image, runs, dsend, drecv,
    s1z, s1x, s1y, r1z, r1x, r1y, s2z, s2x, s2y, r2z, r2x, r2y, s3z, s3x, s3y, r3z, r3x, r3y,
    c3z, c3x, c3y,
    order, table,
    loc, ysem, xsem, zsem, csem, lsem, dsem, sem1, sem2, sem2x, sem3s, sem3r, fsem,
):
    ops, blk = lax.axis_index("ops"), lax.axis_index("blk")
    z, xh, core = ops // 4, (ops // 2) % 2, ops % 2
    y, xl = blk // 2, blk % 2
    x, e = xh * 2 + xl, z % 2

    def device(dz=0, dx=0, dy=0, dc=0):
        zz, xx, yy, cc = (z + dz) % 4, (x + dx) % 4, (y + dy) % 4, (core + dc) % 2
        return (zz * 4 + (xx // 2) * 2 + cc, yy * 2 + xx % 2)

    def mate(dy, flip):
        return (ops, ((y + dy) % 4) * 2 + (xl + flip) % 2)

    sent = []

    def send(src, dst, send_sem, recv_sem, to):
        copy = pltpu.make_async_remote_copy(
            src_ref=src, dst_ref=dst, send_sem=send_sem, recv_sem=recv_sem, device_id=to, device_id_type=MESH
        )
        copy.start()
        sent.append(copy)

    def arrived(dst, sem):
        pltpu.make_async_remote_copy(
            src_ref=dst, dst_ref=dst, send_sem=sem, recv_sem=sem, device_id=device(dc=1), device_id_type=MESH
        ).wait_recv()

    barrier = pltpu.get_barrier_semaphore()
    peers = [device(dc=1)]
    for d in (1, 2, 3):
        peers += [device(dc=c, **{axis: d}) for axis in ("dz", "dx", "dy") for c in range(2)] + [mate(d, 1)]
    for peer in peers:
        pl.semaphore_signal(barrier, inc=1, device_id=peer, device_id_type=MESH)
    in_psi = pltpu.make_async_copy(psi, states.at[pl.ds(blk * 16, 16)], loc.at[0])
    in_left = pltpu.make_async_copy(left, lin, loc.at[1])
    in_right = pltpu.make_async_copy(right, rops, loc.at[2])
    small = [
        pltpu.make_async_copy(a, b, loc.at[4 + n])
        for n, (a, b) in enumerate(((partner_in, partner), (lens_in, lens), (targets_in, targets)))
    ]
    in_psi.start()
    for copy in small:
        copy.start()
    in_left.start()
    in_right.start()

    ys = [0, 3, 1, 2]

    def unit(j, flip, parity, half, k, n=1):
        c = ((y + ys[j]) % 4) * 2 + (xl + flip) % 2
        return states.at[pl.ds(((c * 2 + parity) * 2 + half) * 4 + k, n)]

    mine = lambda j, flip, k, n=1: unit(j, flip, e, core, k, n)

    def y_out(n, j, k, dy):
        send(mine(j, 0, k), mine(j, 0, k), ysem.at[0, n], ysem.at[1, n], device(dy=dy))

    ready = set()

    def x_out(j, k):
        half = k // 2
        ready.add((j, k))
        if (j, k ^ 1) in ready:
            ref = mine(j, 0, half * 2, 2)
            send(ref, ref, xsem.at[0, j, half], xsem.at[1, j, half], device(dx=3 if half else 1))

    seen = set()

    def z_out(flip, j, k):
        n, half = flip * 4 + j, k // 2
        seen.add((n, k))
        if (n, k ^ 1) in seen:
            ref = mine(j, flip, half * 2, 2)
            send(ref, ref, zsem.at[0, n, half], zsem.at[1, n, half], device(dz=3 if half else 1))

    def c_out(flip, j, other):
        n = flip * 4 + j
        ref = unit(j, flip, (e + other) % 2, core, 0, 4)
        send(ref, ref, csem.at[0, n, other], csem.at[1, n, other], device(dc=1))

    def l_out(dy, flip):
        n = dy * 2 + flip
        to = ((y + dy) % 4) * 2 + (xl + flip) % 2
        send(lsend.at[to], lrecv.at[blk], lsem.at[0, n], lsem.at[1, n], mate(dy, flip))

    def images(*blocks):
        at = [(((y + ys[j]) % 4) * 2 + (xl + flip) % 2) * 2 + (e + other) % 2 for flip, j, other in blocks]

        @pl.loop(0, 2)
        def _(i):
            rows = jnp.concatenate([states[pl.ds(q * 8, 8)].reshape(128, 1024) for q in at], axis=0)
            for n in range(4):
                made = jnp.dot(rows, rops[i, :, n * 256 : n * 256 + 256], preferred_element_type=F32).astype(BF16)
                for k in range(2):
                    image[n, i * 16 + at[k]] = made[k * 128 : k * 128 + 128]

    def images_of(*blocks):
        for flip, j, other in blocks:
            arrived(unit(j, flip, (e + other) % 2, (core + 1) % 2, 0, 4), csem.at[1, flip * 4 + j, other])
        images(*blocks)

    for copy in small:
        copy.wait()
    number = lambda cond: jnp.where(cond, 1, 0)
    kk = lax.broadcasted_iota(jnp.int32, (32, 128), 0)
    lane = lax.broadcasted_iota(jnp.int32, (32, 128), 1)
    owners = [lax.rem(partner[blk * 2 + i], 16) for i in range(2)]
    goals = [targets[owners[i], q] for i in range(2) for q in range(16)]
    goal = jnp.zeros((32, 128), jnp.int32)
    for at in range(32):
        goal = jnp.where(kk == at, goals[at], goal)
    key = goal * 32 + kk
    rank, again = jnp.zeros((32, 128), jnp.int32), jnp.zeros((32, 128), jnp.int32)
    for at in range(32):
        rank = rank + number(key > goals[at] * 32 + at)
        again = again + number((goal == goals[at]) & (kk > at))
    place = rank == lane
    left_at = (kk % 16 // 2) * 4 + (kk // 16) * 2 + kk % 2

    def down_sum(value):
        value = value[:8] + value[8:16] + value[16:24] + value[24:]
        return sum(value[r : r + 1] for r in range(1, 8)) + value[:1]

    rows = [
        down_sum(jnp.where(place, kk, 0)), down_sum(jnp.where(place, left_at, 0)),
        down_sum(number(place & (again > 0))), jnp.maximum(down_sum(number(goal <= lane)) - 1, 0),
        jnp.minimum(down_sum(number(goal == lane)), 1), jnp.zeros((3, 128), jnp.int32),
    ]
    order[...] = jnp.concatenate(rows, axis=0)
    order_out = pltpu.make_async_copy(order, table, loc.at[3])

    in_psi.wait()
    pl.semaphore_wait(barrier, len(peers))
    for k in range(4):
        y_out(k, 0, k, 1)
        y_out(7 - k, 0, 3 - k, 3)
        x_out(0, (0, 2, 1, 3)[k])

    in_left.wait()
    lane = lax.broadcasted_iota(jnp.int32, (128, 128), 1)
    masks = [jnp.where(lane < lens[2 * blk + k], 1.0, 0.0).astype(BF16) for k in range(2)]

    @pl.loop(0, 8)
    def _(c):
        for i in range(2):
            for k in range(2):
                lsend[c, i * 2 + k] = lin[lax.rem(partner[c * 2 + i], 16), k] * masks[k]

    lrecv[blk] = lsend[blk]
    l_out(0, 1)
    order_out.start()
    in_right.wait()

    def from_y(j, k, n):
        arrived(mine(j, 0, k), ysem.at[1, n])
        x_out(j, k)
        z_out(0, j, k)

    def near_y(k):
        arrived(mine(1, 0, k), ysem.at[1, k])
        if k < 2:
            y_out(8 + k, 1, k, 1)
        x_out(1, k)
        z_out(0, 1, k)
        m = 3 - k
        arrived(mine(2, 0, m), ysem.at[1, 4 + m])
        if m > 1:
            y_out(8 + m, 2, m, 3)
        x_out(2, m)
        z_out(0, 2, m)

    def from_x(j, k):
        if k % 2 == 0:
            arrived(mine(j, 1, k, 2), xsem.at[1, j, k // 2])
            z_out(1, j, k)
            z_out(1, j, k + 1)

    def from_z(flip, j):
        for k in range(2):
            arrived(unit(j, flip, (e + 1) % 2, core, 2 * k, 2), zsem.at[1, flip * 4 + j, k])
        c_out(flip, j, 1)

    images((0, 0, 0), (0, 0, 1))
    near_y(0)
    near_y(1)
    for k in range(4):
        from_x(0, k)
    c_out(1, 0, 0)
    near_y(2)
    near_y(3)
    c_out(0, 1, 0)
    c_out(0, 2, 0)
    l_out(1, 0)
    l_out(3, 0)
    l_out(2, 0)
    for k in (0, 3, 1, 2):
        from_y(3, k, 8 + k)
    c_out(0, 3, 0)
    for dy in (1, 3, 2):
        l_out(dy, 1)
    images_of((1, 0, 0), (0, 1, 0))
    for k in range(4):
        from_x(1, k)
        from_x(2, 3 - k)
    c_out(1, 1, 0)
    c_out(1, 2, 0)
    from_z(0, 1)
    from_z(0, 2)
    images_of((0, 2, 0), (0, 3, 0))
    for k in (0, 3, 1, 2):
        from_x(3, k)
    c_out(1, 3, 0)
    from_z(1, 0)
    images_of((0, 1, 1), (0, 2, 1))
    from_z(0, 3)
    images_of((1, 1, 0), (1, 2, 0))
    from_z(1, 1)
    from_z(1, 2)
    images_of((1, 0, 1), (0, 3, 1))
    from_z(1, 3)
    images_of((1, 1, 1), (1, 2, 1))
    images_of((1, 3, 0), (1, 3, 1))
    order_out.wait()
    for dy in range(4):
        for flip in range(2):
            if dy or flip:
                source_at = ((y - dy) % 4) * 2 + (xl + flip) % 2
                arrived(lrecv.at[source_at], lsem.at[1, dy * 2 + flip])

    def mix(zi):
        chunk = (z + ZR[zi]) % 4

        def group(g, acc):
            for u in range(GROUP):
                p = g * GROUP + u
                keep = table[2, p].astype(F32)
                acc = acc * keep + jnp.dot(
                    lrecv[table[1, p] // 4, table[1, p] % 4], image[chunk, table[0, p]], preferred_element_type=F32
                )
                runs[zi % 2, p] = acc.astype(BF16)
            return acc

        lax.fori_loop(0, 32 // GROUP, group, jnp.zeros((128, 256), F32))

    def total(zi, t):
        value = runs[zi % 2, table[3, t]].astype(F32)
        return value * table[4, t].astype(F32)

    def swap(zi):
        for half in range(2):

            @pl.loop(half * 4, half * 4 + 4, unroll=True)
            def _(c):
                dsend[zi, c] = total(zi, 2 * c + 1 - core).astype(BF16)

            part = pl.ds(half * 4, 4)
            send(dsend.at[zi, part], drecv.at[zi, part], dsem.at[0, zi, half], dsem.at[1, zi, half], device(dc=1))

    def join(zi):
        def rows_of(yd):
            for xld in range(2):
                c = yd * 2 + xld
                value = (total(zi, 2 * c + core) + drecv[zi, c].astype(F32)).astype(BF16)
                for xhd in range(2):
                    part = value[:, xhd * 128 : xhd * 128 + 128]
                    s1z[zi, (xhd * 2 + xld) * 4 + yd] = part[:PZ]
                    s1x[xhd * 2 + xld, zi, yd] = part[PZ : PZ + PX]
                    s1y[yd, zi, xhd * 2 + xld] = part[PZ + PX :]

        for half in range(2):
            arrived(drecv.at[zi, pl.ds(half * 4, 4)], dsem.at[1, zi, half])
            pl.loop(half * 2, half * 2 + 2, unroll=True)(rows_of)

    def first_out(zi):
        for d in (1, 2, 3):
            send(s1x.at[(x + d) % 4, zi], r1x.at[d - 1, zi], sem1.at[0, 1, d - 1, zi], sem1.at[1, 1, d - 1, zi], device(dx=d))
            send(s1y.at[(y + d) % 4, zi], r1y.at[d - 1, zi], sem1.at[0, 2, d - 1, zi], sem1.at[1, 2, d - 1, zi], device(dy=d))
        if zi < 3:
            send(s1z.at[zi], r1z.at[zi], sem1.at[0, 0, zi, 0], sem1.at[1, 0, zi, 0], device(dz=ZR[zi]))

    for zi in range(4):
        mix(zi)
        swap(zi)
        if zi >= 1:
            join(zi - 1)
            first_out(zi - 1)
    join(3)
    first_out(3)

    def summed(own, others):
        value = own.astype(F32)
        for other in others:
            value = value + other.astype(F32)
        return value

    def second_x(zi):
        for d in range(3):
            arrived(r1x.at[d, zi], sem1.at[1, 1, d, zi])
        for yd in range(4):
            s2x[yd, zi] = summed(s1x[x, zi, yd], [r1x[d, zi, yd] for d in range(3)]).astype(BF16)
        for d in (1, 2, 3):
            send(s2x.at[(y + d) % 4, zi], r2x.at[d - 1, zi], sem2x.at[0, d - 1, zi], sem2x.at[1, d - 1, zi], device(dy=d))

    def second_y(zi):
        for d in range(3):
            arrived(r1y.at[d, zi], sem1.at[1, 2, d, zi])
        for b in range(4):
            s2y[zi, b] = summed(s1y[y, zi, b], [r1y[d, zi, b] for d in range(3)]).astype(BF16)
        if zi < 3:
            send(s2y.at[zi], r2y.at[zi], sem2.at[0, 1, zi], sem2.at[1, 1, zi], device(dz=ZR[zi]))

    def second_z():
        for d in range(3):
            arrived(r1z.at[d], sem1.at[1, 0, d, 0])
        for xd in range(4):
            for yd in range(4):
                b = xd * 4 + yd
                s2z[xd, yd] = summed(s1z[3, b], [r1z[d, b] for d in range(3)]).astype(BF16)
        for d in (1, 2, 3):
            send(s2z.at[(x + d) % 4], r2z.at[d - 1], sem2.at[0, 0, d - 1], sem2.at[1, 0, d - 1], device(dx=d))

    def third_out(part, src, dst, d, axis):
        for dc in range(2):
            send(src, dst.at[core, d - 1], sem3s.at[part, dc, d - 1], sem3r.at[part, core, d - 1], device(**{axis: ZR[d - 1] if axis == "dz" else d, "dc": dc}))

    def third_own(part, src, dst):
        send(src, dst, fsem.at[0, part], fsem.at[1, part], device(dc=1))

    def third_x(zi):
        for d in range(3):
            arrived(r2x.at[d, zi], sem2x.at[1, d, zi])
        s3x[zi] = summed(s2x[y, zi], [r2x[d, zi] for d in range(3)]).astype(BF16)
        if zi < 3:
            third_out(1, s3x.at[zi], r3x, zi + 1, "dz")
        else:
            third_own(1, s3x.at[3], c3x)

    second_x(0)
    second_y(0)
    second_x(1)
    second_y(1)
    second_z()
    second_x(2)
    second_y(2)
    third_x(0)
    second_x(3)
    second_y(3)
    third_x(1)
    for d in range(3):
        arrived(r2z.at[d], sem2.at[1, 0, d])
    for yd in range(4):
        s3z[yd] = summed(s2z[x, yd], [r2z[d, yd] for d in range(3)]).astype(BF16)
    for d in (1, 2, 3):
        third_out(0, s3z.at[(y + d) % 4], r3z, d, "dy")
    third_own(0, s3z.at[y], c3z)
    third_x(2)
    for d in range(3):
        arrived(r2y.at[d], sem2.at[1, 1, d])
    for b in range(4):
        s3y[b] = summed(s2y[3, b], [r2y[d, b] for d in range(3)]).astype(BF16)
    for d in (1, 2, 3):
        third_out(2, s3y.at[(x + d) % 4], r3y, d, "dx")
    third_own(2, s3y.at[x], c3y)
    third_x(3)

    row = lax.broadcasted_iota(jnp.int32, (128, 128), 0)
    for part, (got, own) in enumerate(((r3z, c3z), (r3x, c3x), (r3y, c3y))):
        for d in range(3):
            for half in range(2):
                arrived(got.at[half, d], sem3r.at[part, half, d])
        arrived(own, fsem.at[1, part])
    for other in range(2):
        half = (core + other) % 2
        own = (c3z[...], c3x[...], c3y[...]) if other else (s3z[y], s3x[3], s3y[x])
        parts = [summed(a, [got[half, d] for d in range(3)]) for a, got in zip(own, (r3z, r3x, r3y))]
        value = jnp.where(row < lens[2 * blk + half], jnp.concatenate(parts, axis=0), 0.0)
        turned = value.T
        out[:, pl.ds(pl.multiple_of(half * 128, 128), 128)] = jnp.where(core == 0, turned[:64], turned[64:]).astype(BF16)
    for copy in sent:
        copy.wait_send()


def local(psi, left_blocks, right_ops, block_target, left_partner, block_len):
    hbm = pl.BlockSpec(memory_space=pl.ANY)
    b = lambda *shape: VMEM(shape, BF16)
    return pl.pallas_call(
        kernel,
        name="sigma",
        out_shape=jax.ShapeDtypeStruct((64, 256), BF16),
        in_specs=[hbm] * 6,
        out_specs=pl.BlockSpec(memory_space=VMEM),
        scratch_shapes=[
            SMEM((16,), jnp.int32), SMEM((16,), jnp.int32), SMEM((16, 16), jnp.int32),
            b(128, 16, 1024), b(8, 4, 128, 128), b(8, 4, 128, 128), b(16, 2, 128, 128), b(2, 1024, 1024),
            b(4, 32, 128, 256), b(2, 32, 128, 256), b(4, 8, 128, 256), b(4, 8, 128, 256),
            b(4, 16, PZ, 128), b(4, 4, 4, PX, 128), b(4, 4, 4, PY, 128),
            b(3, 16, PZ, 128), b(3, 4, 4, PX, 128), b(3, 4, 4, PY, 128),
            b(4, 4, PZ, 128), b(4, 4, PX, 128), b(4, 4, PY, 128),
            b(3, 4, PZ, 128), b(3, 4, PX, 128), b(3, 4, PY, 128),
            b(4, PZ, 128), b(4, PX, 128), b(4, PY, 128),
            b(2, 3, PZ, 128), b(2, 3, PX, 128), b(2, 3, PY, 128),
            b(PZ, 128), b(PX, 128), b(PY, 128),
            VMEM((8, 128), jnp.int32), SMEM((8, 128), jnp.int32),
            DMA((7,)), DMA((2, 12)), DMA((2, 4, 2)), DMA((2, 8, 2)), DMA((2, 8, 2)), DMA((2, 8)), DMA((2, 4, 2)),
            DMA((2, 3, 3, 4)), DMA((2, 2, 3)), DMA((2, 3, 4)), DMA((3, 2, 3)), DMA((3, 2, 3)), DMA((2, 3)),
        ],
        compiler_params=pltpu.CompilerParams(
            collective_id=0, has_side_effects=True, vmem_limit_bytes=60 << 20
        ),
    )(left_partner, block_len, block_target, psi.reshape(16, 16, 1024), left_blocks, right_ops).T


def solution(mesh):
    return jax.shard_map(
        local,
        mesh=mesh,
        in_specs=(
            P("blk", None),
            P("ops", "blk", None, None),
            P(("ops", "blk"), None, None),
            P("ops", None),
            P("ops"),
            P(),
        ),
        out_specs=P("blk", "ops"),
        check_vma=False,
    )
```

```python
import jax
import jax.numpy as jnp
from jax import lax
from jax.experimental import pallas as pl
from jax.experimental.pallas import tpu as pltpu
from jax.sharding import PartitionSpec as P

MESH = pl.DeviceIdType.MESH
F32, BF16 = jnp.float32, jnp.bfloat16
VMEM, SMEM, DMA = pltpu.VMEM, pltpu.SMEM, pltpu.SemaphoreType.DMA
PZ, PX, PY = 32, 48, 48
GROUP = 32
ZR = (1, 3, 2, 0)


def kernel(
    partner_in, lens_in, targets_in, psi, left, right, out,
    partner, lens, targets,
    states, lsend, lrecv, lin, rops, image, runs, dsend, drecv,
    s1z, s1x, s1y, r1z, r1x, r1y, s2z, s2x, s2y, r2z, r2x, r2y, s3z, s3x, s3y, r3z, r3x, r3y,
    c3z, c3x, c3y,
    order, table,
    loc, ysem, xsem, zsem, csem, lsem, dsem, sem1, sem2, sem2x, sem3s, sem3r, fsem,
):
    ops, blk = lax.axis_index("ops"), lax.axis_index("blk")
    z, xh, core = ops // 4, (ops // 2) % 2, ops % 2
    y, xl = blk // 2, blk % 2
    x, e = xh * 2 + xl, z % 2

    def device(dz=0, dx=0, dy=0, dc=0):
        zz, xx, yy, cc = (z + dz) % 4, (x + dx) % 4, (y + dy) % 4, (core + dc) % 2
        return (zz * 4 + (xx // 2) * 2 + cc, yy * 2 + xx % 2)

    def mate(dy, flip):
        return (ops, ((y + dy) % 4) * 2 + (xl + flip) % 2)

    sent = []

    def send(src, dst, send_sem, recv_sem, to):
        copy = pltpu.make_async_remote_copy(
            src_ref=src, dst_ref=dst, send_sem=send_sem, recv_sem=recv_sem, device_id=to, device_id_type=MESH
        )
        copy.start()
        sent.append(copy)

    def arrived(dst, sem):
        pltpu.make_async_remote_copy(
            src_ref=dst, dst_ref=dst, send_sem=sem, recv_sem=sem, device_id=device(dc=1), device_id_type=MESH
        ).wait_recv()

    barrier = pltpu.get_barrier_semaphore()
    peers = [device(dc=1)]
    for d in (1, 2, 3):
        peers += [device(dc=c, **{axis: d}) for axis in ("dz", "dx", "dy") for c in range(2)] + [mate(d, 1)]
    for peer in peers:
        pl.semaphore_signal(barrier, inc=1, device_id=peer, device_id_type=MESH)
    in_psi = pltpu.make_async_copy(psi, states.at[pl.ds(blk * 16, 16)], loc.at[0])
    in_left = pltpu.make_async_copy(left, lin, loc.at[1])
    in_right = pltpu.make_async_copy(right, rops, loc.at[2])
    small = [
        pltpu.make_async_copy(a, b, loc.at[4 + n])
        for n, (a, b) in enumerate(((partner_in, partner), (lens_in, lens), (targets_in, targets)))
    ]
    in_psi.start()
    for copy in small:
        copy.start()
    in_left.start()
    in_right.start()

    ys = [0, 3, 1, 2]

    def unit(j, flip, parity, half, k, n=1):
        c = ((y + ys[j]) % 4) * 2 + (xl + flip) % 2
        return states.at[pl.ds(((c * 2 + parity) * 2 + half) * 4 + k, n)]

    mine = lambda j, flip, k, n=1: unit(j, flip, e, core, k, n)

    def y_out(n, j, k, dy):
        send(mine(j, 0, k), mine(j, 0, k), ysem.at[0, n], ysem.at[1, n], device(dy=dy))

    ready = set()

    def x_out(j, k):
        half = k // 2
        ready.add((j, k))
        if (j, k ^ 1) in ready:
            ref = mine(j, 0, half * 2, 2)
            send(ref, ref, xsem.at[0, j, half], xsem.at[1, j, half], device(dx=3 if half else 1))

    seen = set()

    def z_out(flip, j, k):
        n, half = flip * 4 + j, k // 2
        seen.add((n, k))
        if (n, k ^ 1) in seen:
            ref = mine(j, flip, half * 2, 2)
            send(ref, ref, zsem.at[0, n, half], zsem.at[1, n, half], device(dz=3 if half else 1))

    def c_out(flip, j, other):
        n = flip * 4 + j
        ref = unit(j, flip, (e + other) % 2, core, 0, 4)
        send(ref, ref, csem.at[0, n, other], csem.at[1, n, other], device(dc=1))

    def l_out(dy, flip):
        n = dy * 2 + flip
        to = ((y + dy) % 4) * 2 + (xl + flip) % 2
        send(lsend.at[to], lrecv.at[blk], lsem.at[0, n], lsem.at[1, n], mate(dy, flip))

    def images(*blocks):
        at = [(((y + ys[j]) % 4) * 2 + (xl + flip) % 2) * 2 + (e + other) % 2 for flip, j, other in blocks]

        @pl.loop(0, 2)
        def _(i):
            rows = jnp.concatenate([states[pl.ds(q * 8, 8)].reshape(128, 1024) for q in at], axis=0)
            for n in range(4):
                made = jnp.dot(rows, rops[i, :, n * 256 : n * 256 + 256], preferred_element_type=F32).astype(BF16)
                for k in range(2):
                    image[n, i * 16 + at[k]] = made[k * 128 : k * 128 + 128]

    def images_of(*blocks):
        for flip, j, other in blocks:
            arrived(unit(j, flip, (e + other) % 2, (core + 1) % 2, 0, 4), csem.at[1, flip * 4 + j, other])
        images(*blocks)

    for copy in small:
        copy.wait()
    number = lambda cond: jnp.where(cond, 1, 0)
    kk = lax.broadcasted_iota(jnp.int32, (32, 128), 0)
    lane = lax.broadcasted_iota(jnp.int32, (32, 128), 1)
    owners = [lax.rem(partner[blk * 2 + i], 16) for i in range(2)]
    goals = [targets[owners[i], q] for i in range(2) for q in range(16)]
    goal = jnp.zeros((32, 128), jnp.int32)
    for at in range(32):
        goal = jnp.where(kk == at, goals[at], goal)
    key = goal * 32 + kk
    rank, again = jnp.zeros((32, 128), jnp.int32), jnp.zeros((32, 128), jnp.int32)
    for at in range(32):
        rank = rank + number(key > goals[at] * 32 + at)
        again = again + number((goal == goals[at]) & (kk > at))
    place = rank == lane
    left_at = (kk % 16 // 2) * 4 + (kk // 16) * 2 + kk % 2

    def down_sum(value):
        value = value[:8] + value[8:16] + value[16:24] + value[24:]
        return sum(value[r : r + 1] for r in range(1, 8)) + value[:1]

    rows = [
        down_sum(jnp.where(place, kk, 0)), down_sum(jnp.where(place, left_at, 0)),
        down_sum(number(place & (again > 0))), jnp.maximum(down_sum(number(goal <= lane)) - 1, 0),
        jnp.minimum(down_sum(number(goal == lane)), 1), jnp.zeros((3, 128), jnp.int32),
    ]
    order[...] = jnp.concatenate(rows, axis=0)
    order_out = pltpu.make_async_copy(order, table, loc.at[3])

    in_psi.wait()
    pl.semaphore_wait(barrier, len(peers))
    for k in range(4):
        y_out(k, 0, k, 1)
        y_out(7 - k, 0, 3 - k, 3)
        x_out(0, (0, 2, 1, 3)[k])

    in_left.wait()
    lane = lax.broadcasted_iota(jnp.int32, (128, 128), 1)
    masks = [jnp.where(lane < lens[2 * blk + k], 1.0, 0.0).astype(BF16) for k in range(2)]

    @pl.loop(0, 8)
    def _(c):
        for i in range(2):
            for k in range(2):
                lsend[c, i * 2 + k] = lin[lax.rem(partner[c * 2 + i], 16), k] * masks[k]

    lrecv[blk] = lsend[blk]
    l_out(0, 1)
    order_out.start()
    in_right.wait()

    def from_y(j, k, n):
        arrived(mine(j, 0, k), ysem.at[1, n])
        x_out(j, k)
        z_out(0, j, k)

    def near_y(k):
        arrived(mine(1, 0, k), ysem.at[1, k])
        if k < 2:
            y_out(8 + k, 1, k, 1)
        x_out(1, k)
        z_out(0, 1, k)
        m = 3 - k
        arrived(mine(2, 0, m), ysem.at[1, 4 + m])
        if m > 1:
            y_out(8 + m, 2, m, 3)
        x_out(2, m)
        z_out(0, 2, m)

    def from_x(j, k):
        if k % 2 == 0:
            arrived(mine(j, 1, k, 2), xsem.at[1, j, k // 2])
            z_out(1, j, k)
            z_out(1, j, k + 1)

    def from_z(flip, j):
        for k in range(2):
            arrived(unit(j, flip, (e + 1) % 2, core, 2 * k, 2), zsem.at[1, flip * 4 + j, k])
        c_out(flip, j, 1)

    images((0, 0, 0), (0, 0, 1))
    near_y(0)
    near_y(1)
    for k in range(4):
        from_x(0, k)
    c_out(1, 0, 0)
    near_y(2)
    near_y(3)
    c_out(0, 1, 0)
    c_out(0, 2, 0)
    l_out(1, 0)
    l_out(3, 0)
    l_out(2, 0)
    for k in (0, 3, 1, 2):
        from_y(3, k, 8 + k)
    c_out(0, 3, 0)
    for dy in (1, 3, 2):
        l_out(dy, 1)
    images_of((1, 0, 0), (0, 1, 0))
    for k in range(4):
        from_x(1, k)
        from_x(2, 3 - k)
    c_out(1, 1, 0)
    c_out(1, 2, 0)
    from_z(0, 1)
    from_z(0, 2)
    images_of((0, 2, 0), (0, 3, 0))
    for k in (0, 3, 1, 2):
        from_x(3, k)
    c_out(1, 3, 0)
    from_z(1, 0)
    images_of((0, 1, 1), (0, 2, 1))
    from_z(0, 3)
    images_of((1, 1, 0), (1, 2, 0))
    from_z(1, 1)
    from_z(1, 2)
    images_of((1, 0, 1), (0, 3, 1))
    from_z(1, 3)
    images_of((1, 1, 1), (1, 2, 1))
    images_of((1, 3, 0), (1, 3, 1))
    order_out.wait()
    for dy in range(4):
        for flip in range(2):
            if dy or flip:
                source_at = ((y - dy) % 4) * 2 + (xl + flip) % 2
                arrived(lrecv.at[source_at], lsem.at[1, dy * 2 + flip])

    def mix(zi):
        chunk = (z + ZR[zi]) % 4

        def group(g, acc):
            for u in range(GROUP):
                p = g * GROUP + u
                keep = table[2, p].astype(F32)
                acc = acc * keep + jnp.dot(
                    lrecv[table[1, p] // 4, table[1, p] % 4], image[chunk, table[0, p]], preferred_element_type=F32
                )
                runs[zi % 2, p] = acc.astype(BF16)
            return acc

        lax.fori_loop(0, 32 // GROUP, group, jnp.zeros((128, 256), F32))

    def total(zi, t):
        value = runs[zi % 2, table[3, t]].astype(F32)
        return value * table[4, t].astype(F32)

    def swap(zi):
        for half in range(2):

            @pl.loop(half * 4, half * 4 + 4, unroll=True)
            def _(c):
                t = 2 * c + 1 - core
                value = runs[zi % 2, table[3, t]]
                dsend[zi, c] = jnp.where(table[4, t] > 0, value, jnp.zeros_like(value))

            part = pl.ds(half * 4, 4)
            send(dsend.at[zi, part], drecv.at[zi, part], dsem.at[0, zi, half], dsem.at[1, zi, half], device(dc=1))

    def join(zi):
        def rows_of(yd):
            for xld in range(2):
                c = yd * 2 + xld
                value = (total(zi, 2 * c + core) + drecv[zi, c].astype(F32)).astype(BF16)
                for xhd in range(2):
                    part = value[:, xhd * 128 : xhd * 128 + 128]
                    s1z[zi, (xhd * 2 + xld) * 4 + yd] = part[:PZ]
                    s1x[xhd * 2 + xld, zi, yd] = part[PZ : PZ + PX]
                    s1y[yd, zi, xhd * 2 + xld] = part[PZ + PX :]

        for half in range(2):
            arrived(drecv.at[zi, pl.ds(half * 4, 4)], dsem.at[1, zi, half])
            pl.loop(half * 2, half * 2 + 2, unroll=True)(rows_of)

    def first_out(zi):
        for d in (1, 2, 3):
            send(s1x.at[(x + d) % 4, zi], r1x.at[d - 1, zi], sem1.at[0, 1, d - 1, zi], sem1.at[1, 1, d - 1, zi], device(dx=d))
            send(s1y.at[(y + d) % 4, zi], r1y.at[d - 1, zi], sem1.at[0, 2, d - 1, zi], sem1.at[1, 2, d - 1, zi], device(dy=d))
        if zi < 3:
            send(s1z.at[zi], r1z.at[zi], sem1.at[0, 0, zi, 0], sem1.at[1, 0, zi, 0], device(dz=ZR[zi]))

    for zi in range(4):
        mix(zi)
        swap(zi)
        if zi >= 1:
            join(zi - 1)
            first_out(zi - 1)
    join(3)
    first_out(3)

    def summed(own, others):
        value = own.astype(F32)
        for other in others:
            value = value + other.astype(F32)
        return value

    def second_x(zi):
        for d in range(3):
            arrived(r1x.at[d, zi], sem1.at[1, 1, d, zi])
        for yd in range(4):
            s2x[yd, zi] = summed(s1x[x, zi, yd], [r1x[d, zi, yd] for d in range(3)]).astype(BF16)
        for d in (1, 2, 3):
            send(s2x.at[(y + d) % 4, zi], r2x.at[d - 1, zi], sem2x.at[0, d - 1, zi], sem2x.at[1, d - 1, zi], device(dy=d))

    def second_y(zi):
        for d in range(3):
            arrived(r1y.at[d, zi], sem1.at[1, 2, d, zi])
        for b in range(4):
            s2y[zi, b] = summed(s1y[y, zi, b], [r1y[d, zi, b] for d in range(3)]).astype(BF16)
        if zi < 3:
            send(s2y.at[zi], r2y.at[zi], sem2.at[0, 1, zi], sem2.at[1, 1, zi], device(dz=ZR[zi]))

    def second_z():
        for d in range(3):
            arrived(r1z.at[d], sem1.at[1, 0, d, 0])
        for xd in range(4):
            for yd in range(4):
                b = xd * 4 + yd
                s2z[xd, yd] = summed(s1z[3, b], [r1z[d, b] for d in range(3)]).astype(BF16)
        for d in (1, 2, 3):
            send(s2z.at[(x + d) % 4], r2z.at[d - 1], sem2.at[0, 0, d - 1], sem2.at[1, 0, d - 1], device(dx=d))

    def third_out(part, src, dst, d, axis):
        for dc in range(2):
            send(src, dst.at[core, d - 1], sem3s.at[part, dc, d - 1], sem3r.at[part, core, d - 1], device(**{axis: ZR[d - 1] if axis == "dz" else d, "dc": dc}))

    def third_own(part, src, dst):
        send(src, dst, fsem.at[0, part], fsem.at[1, part], device(dc=1))

    def third_x(zi):
        for d in range(3):
            arrived(r2x.at[d, zi], sem2x.at[1, d, zi])
        s3x[zi] = summed(s2x[y, zi], [r2x[d, zi] for d in range(3)]).astype(BF16)
        if zi < 3:
            third_out(1, s3x.at[zi], r3x, zi + 1, "dz")
        else:
            third_own(1, s3x.at[3], c3x)

    second_x(0)
    second_y(0)
    second_x(1)
    second_y(1)
    second_z()
    second_x(2)
    second_y(2)
    third_x(0)
    second_x(3)
    second_y(3)
    third_x(1)
    for d in range(3):
        arrived(r2z.at[d], sem2.at[1, 0, d])
    for yd in range(4):
        s3z[yd] = summed(s2z[x, yd], [r2z[d, yd] for d in range(3)]).astype(BF16)
    for d in (1, 2, 3):
        third_out(0, s3z.at[(y + d) % 4], r3z, d, "dy")
    third_own(0, s3z.at[y], c3z)
    third_x(2)
    for d in range(3):
        arrived(r2y.at[d], sem2.at[1, 1, d])
    for b in range(4):
        s3y[b] = summed(s2y[3, b], [r2y[d, b] for d in range(3)]).astype(BF16)
    for d in (1, 2, 3):
        third_out(2, s3y.at[(x + d) % 4], r3y, d, "dx")
    third_own(2, s3y.at[x], c3y)
    third_x(3)

    row = lax.broadcasted_iota(jnp.int32, (128, 128), 0)
    for part, (got, own) in enumerate(((r3z, c3z), (r3x, c3x), (r3y, c3y))):
        for d in range(3):
            for half in range(2):
                arrived(got.at[half, d], sem3r.at[part, half, d])
        arrived(own, fsem.at[1, part])
    for other in range(2):
        half = (core + other) % 2
        own = (c3z[...], c3x[...], c3y[...]) if other else (s3z[y], s3x[3], s3y[x])
        parts = [summed(a, [got[half, d] for d in range(3)]) for a, got in zip(own, (r3z, r3x, r3y))]
        value = jnp.where(row < lens[2 * blk + half], jnp.concatenate(parts, axis=0), 0.0)
        turned = value.T
        out[:, pl.ds(pl.multiple_of(half * 128, 128), 128)] = jnp.where(core == 0, turned[:64], turned[64:]).astype(BF16)
    for copy in sent:
        copy.wait_send()


def local(psi, left_blocks, right_ops, block_target, left_partner, block_len):
    hbm = pl.BlockSpec(memory_space=pl.ANY)
    b = lambda *shape: VMEM(shape, BF16)
    return pl.pallas_call(
        kernel,
        name="sigma",
        out_shape=jax.ShapeDtypeStruct((64, 256), BF16),
        in_specs=[hbm] * 6,
        out_specs=pl.BlockSpec(memory_space=VMEM),
        scratch_shapes=[
            SMEM((16,), jnp.int32), SMEM((16,), jnp.int32), SMEM((16, 16), jnp.int32),
            b(128, 16, 1024), b(8, 4, 128, 128), b(8, 4, 128, 128), b(16, 2, 128, 128), b(2, 1024, 1024),
            b(4, 32, 128, 256), b(2, 32, 128, 256), b(4, 8, 128, 256), b(4, 8, 128, 256),
            b(4, 16, PZ, 128), b(4, 4, 4, PX, 128), b(4, 4, 4, PY, 128),
            b(3, 16, PZ, 128), b(3, 4, 4, PX, 128), b(3, 4, 4, PY, 128),
            b(4, 4, PZ, 128), b(4, 4, PX, 128), b(4, 4, PY, 128),
            b(3, 4, PZ, 128), b(3, 4, PX, 128), b(3, 4, PY, 128),
            b(4, PZ, 128), b(4, PX, 128), b(4, PY, 128),
            b(2, 3, PZ, 128), b(2, 3, PX, 128), b(2, 3, PY, 128),
            b(PZ, 128), b(PX, 128), b(PY, 128),
            VMEM((8, 128), jnp.int32), SMEM((8, 128), jnp.int32),
            DMA((7,)), DMA((2, 12)), DMA((2, 4, 2)), DMA((2, 8, 2)), DMA((2, 8, 2)), DMA((2, 8)), DMA((2, 4, 2)),
            DMA((2, 3, 3, 4)), DMA((2, 2, 3)), DMA((2, 3, 4)), DMA((3, 2, 3)), DMA((3, 2, 3)), DMA((2, 3)),
        ],
        compiler_params=pltpu.CompilerParams(
            collective_id=0, has_side_effects=True, vmem_limit_bytes=60 << 20
        ),
    )(left_partner, block_len, block_target, psi.reshape(16, 16, 1024), left_blocks, right_ops).T


def solution(mesh):
    return jax.shard_map(
        local,
        mesh=mesh,
        in_specs=(
            P("blk", None),
            P("ops", "blk", None, None),
            P(("ops", "blk"), None, None),
            P("ops", None),
            P("ops"),
            P(),
        ),
        out_specs=P("blk", "ops"),
        check_vma=False,
    )
```
